32 devices in a mesh: filt: 4 (over y, x), dom: 8 (over z, core).
Axes of the slice: x: 2, y: 2, z: 4, core: 2. Of those that a mesh axis runs over, the one named last changes fastest.
Arguments:
- log_weights: float32 [524288], P(('filt', 'dom')), parts along dimension 0, may hold values from -20 to 250, as said below
- bins: int32 [524288], P(('filt', 'dom')), parts along dimension 0, may hold values from 0 to 4095
- states: bfloat16 [128, 524288], P(None, ('filt', 'dom')), parts along dimension 1, may hold values from -6 to 6
Outputs:
- cumulative: float32 [16384], P(('filt', 'dom')), parts along dimension 0
- bin_means: float32 [128, 16384], P(None, ('filt', 'dom')), parts along dimension 1
- particle_weights: float32 [524288], P(('filt', 'dom')), parts along dimension 0
The draws below stay inside these ranges and needn't reach their ends.
There are 4 independent parts, one for each index of `filt`. The reference program is written for one: setup_inputs(seed, part) draws one part's arguments, and reference() takes and returns one part's arrays. A program takes and returns all parts, laid end to end along the dimension named above; each array names one. Nothing has to cross between parts.
Inputs may be any that keep to these rules, and one draw needn't show every extreme that they name: `log_weights`: finite log-weights.
All inputs are finite; a program needn't handle non-finite values.
Results may differ from the reference program's by a relative error of at most 0.00051.
Values sent between devices are 32-bit elements; how exact they have to be, the bound alone decides.
A program may use at most 64 MiB of HBM per device.

```python
import math
import jax
import jax.numpy as jnp
import numpy as np
from jax import lax

BINS = 4096
STATE = 128
P_DEV = 16384
PARTICLES = 131072
N_DOM = 8


def draw_log_weights(key, part):
    key_offset, key_noise = jax.random.split(jax.random.fold_in(key, 7))
    groups = PARTICLES // P_DEV
    offsets = jax.random.uniform(key_offset, (groups,), jnp.float32, -3.0, 3.0)
    noise = jnp.clip(1.5 * jax.random.normal(key_noise, (groups, P_DEV), jnp.float32), -8.0, 8.0)
    return (offsets[:, None] + noise).reshape(PARTICLES).astype(jnp.float32)


def set_ends(entries, stream_key, least, top_value):
    dims = entries.shape
    spot = [jax.random.randint(jax.random.fold_in(stream_key, axis), (), 0, dims[axis]) for axis in range(len(dims))]
    entries = entries.at[tuple(spot)].set(least)
    longest = dims.index(max(dims))
    spot[longest] = (spot[longest] + 1) % dims[longest]
    return entries.at[tuple(spot)].set(top_value)


def level_of(rng, dims, cuts, smallest, largest):
    gain = 1.0
    for axis_at, blocks in cuts:
        heights = jax.random.uniform(jax.random.fold_in(jax.random.fold_in(rng, 6), axis_at), (blocks,), jnp.float32, smallest / len(cuts), largest / len(cuts))
        gain = gain * jnp.repeat(jnp.exp(heights), dims[axis_at] // blocks).reshape((-1,) + (1,) * (len(dims) - 1 - axis_at))
    return gain


def rank_bounds(count, slope):
    weights = [(1 << 20) // math.isqrt(grade ** slope) + 1 for grade in range(1, count + 1)]
    scale = 1 + sum(weights) // (1 << 30)
    return np.cumsum(np.array([max(1, weight // scale) for weight in weights]))


def ranked(key, extent, amount, lean):
    table = rank_bounds(amount, lean)
    pick = jax.random.randint(jax.random.fold_in(key, 1), extent, 0, int(table[amount - 1]))
    rank = jnp.searchsorted(jnp.asarray(table, jnp.int32), pick, side="right")
    return jax.random.permutation(jax.random.fold_in(key, 2), amount)[rank].astype(jnp.int32)


def scatter_about(stream_key, dims, scale, limit, pieces=(), held_as=jnp.bfloat16):
    level = level_of(stream_key, dims, pieces, -0.22, 0.18) if pieces else 1.0
    entries = jax.random.normal(stream_key, dims, jnp.float32) * scale * level
    return jnp.minimum(jnp.maximum(entries, -limit), limit).astype(held_as)


def setup_inputs(seed: int = 0, part: int = 0) -> dict:
    key_of = jax.random.split(jax.random.key(seed), 4)
    part_splits = jax.random.split(jax.random.fold_in(key_of[3], part), 4)
    log_weights = draw_log_weights(jax.random.fold_in(jax.random.fold_in(key_of[3], part), 71), part)
    bins = set_ends(ranked(part_splits[1], (PARTICLES,), BINS, 2), jax.random.fold_in(part_splits[1], 3), 0, BINS - 1).astype(jnp.int32)
    states = scatter_about(part_splits[2], (STATE, PARTICLES), 1.0, 6.0, ((1, 8),))
    return dict(log_weights=log_weights, bins=bins, states=states)


floor_value = -1.0e4


def group_pairs(group_weights, group_bins, group_states):
    width = min(P_DEV, 1024)
    blocks = P_DEV // width
    labels = lax.iota(jnp.int32, BINS)

    def top_step(index, carry):
        start = (index * width).astype(jnp.int32)
        row_weights = lax.dynamic_slice_in_dim(group_weights, start, width)
        row_bins = lax.dynamic_slice_in_dim(group_bins, start, width)
        member = row_bins[:, None] == labels[None, :]
        return jnp.maximum(carry, jnp.max(jnp.where(member, row_weights[:, None], floor_value), axis=0))

    bin_top = lax.fori_loop(0, blocks, top_step, jnp.full((BINS,), floor_value, jnp.float32))

    def sum_step(index, carry):
        totals, sums = carry
        start = (index * width).astype(jnp.int32)
        row_weights = lax.dynamic_slice_in_dim(group_weights, start, width)
        row_bins = lax.dynamic_slice_in_dim(group_bins, start, width)
        row_states = lax.dynamic_slice_in_dim(group_states, start, width, 1).astype(jnp.float32)
        member = row_bins[:, None] == labels[None, :]
        own_top = jnp.sum(jnp.where(member, bin_top[None, :], jnp.float32(0.0)), axis=1)
        scaled = jnp.exp(row_weights - own_top).astype(jnp.bfloat16).astype(jnp.float32)
        spread = jnp.where(member, scaled[:, None], jnp.float32(0.0))
        totals = totals + jnp.sum(spread, axis=0)
        sums = sums + jnp.dot(row_states, spread, precision=lax.Precision.HIGHEST, preferred_element_type=jnp.float32)
        return totals, sums

    start_pair = (jnp.zeros((BINS,), jnp.float32), jnp.zeros((STATE, BINS), jnp.float32))
    totals, sums = lax.fori_loop(0, blocks, sum_step, start_pair)
    return bin_top, totals, sums


def reference(log_weights, bins, states):
    def one_group(group):
        start = (group * P_DEV).astype(jnp.int32)
        return group_pairs(lax.dynamic_slice_in_dim(log_weights, start, P_DEV),
                           lax.dynamic_slice_in_dim(bins, start, P_DEV),
                           lax.dynamic_slice_in_dim(states, start, P_DEV, 1))

    local_top, local_mass, local_sums = lax.map(one_group, jnp.arange(N_DOM, dtype=jnp.int32))
    bin_top = jnp.max(local_top, axis=0)
    factor = jnp.exp(local_top - bin_top[None, :])
    bin_mass = jnp.sum(local_mass * factor, axis=0)
    bin_sums = jnp.sum(local_sums * factor[:, None, :], axis=0)
    top = jnp.max(bin_top)
    share = bin_mass * jnp.exp(bin_top - top)
    total = jnp.sum(share)
    cumulative = jnp.cumsum(share) / total
    bin_means = bin_sums / jnp.maximum(bin_mass, 1.0)[None, :]
    particle_weights = (P_DEV * N_DOM) * jnp.exp(log_weights - top) / total
    return cumulative, bin_means, particle_weights
```

```python
import functools

import jax
import jax.numpy as jnp
from jax import lax
from jax.experimental import pallas as pl
from jax.experimental.pallas import tpu as pltpu
from jax.sharding import PartitionSpec as P

BINS = 4096
LANES = 128
EXTRA = 16

floor_value = -10000.0


def spread_rows(ref, values):
    for r in range(values.shape[0]):
        ref[16 * r:16 * r + 16, :] = jnp.broadcast_to(values[r:r + 1, :], (16, LANES)).astype(ref.dtype)


def sort_pairs(keys, values):
    tile_bits = len(keys).bit_length() - 1
    bits = tile_bits + 10
    sub = lax.broadcasted_iota(jnp.int32, (8, LANES), 0)
    lane = lax.broadcasted_iota(jnp.int32, (8, LANES), 1)

    def mask_of(bit):
        if bit < tile_bits + 3:
            return (sub & (1 << (bit - tile_bits))) != 0
        return (lane & (1 << (bit - tile_bits - 3))) != 0

    def after(ka, va, kb, vb):
        return (ka > kb) | ((ka == kb) & (va > vb))

    for size in range(1, bits + 1):
        for bit in range(size - 1, -1, -1):
            down = mask_of(size) if tile_bits <= size < bits else None
            if bit < tile_bits:
                for t in range(len(keys)):
                    o = t | (1 << bit)
                    if o == t:
                        continue
                    swap = after(keys[t], values[t], keys[o], values[o])
                    if down is not None:
                        swap = jnp.logical_xor(swap, down)
                    elif size < tile_bits and t & (1 << size):
                        swap = after(keys[o], values[o], keys[t], values[t])
                    keys[t], keys[o] = jnp.where(swap, keys[o], keys[t]), jnp.where(swap, keys[t], keys[o])
                    values[t], values[o] = (jnp.where(swap, values[o], values[t]),
                                            jnp.where(swap, values[t], values[o]))
                continue
            upper = mask_of(bit)
            turn = upper if down is None else jnp.logical_xor(upper, down)
            if bit < tile_bits + 3:
                hop = 1 << (bit - tile_bits)

                def partner(x):
                    if 2 * hop == 8:
                        return pltpu.roll(x, hop, 0)
                    return jnp.where(upper, pltpu.roll(x, hop, 0), pltpu.roll(x, 8 - hop, 0))
            else:
                index = lane ^ (1 << (bit - tile_bits - 3))

                def partner(x):
                    return jnp.take_along_axis(x, index, axis=1)
            for t in range(len(keys)):
                k, v = partner(keys[t]), partner(values[t])
                swap = jnp.logical_xor(after(keys[t], values[t], k, v), turn)
                keys[t] = jnp.where(swap, k, keys[t])
                values[t] = jnp.where(swap, v, values[t])
    return keys, values


def local_tops(lw, bins):
    count = lw.shape[0] // 8
    table = BINS // LANES
    keys, values = sort_pairs([bins[8 * t:8 * t + 8] for t in range(count)],
                              [lw[8 * t:8 * t + 8] for t in range(count)])
    sub = lax.broadcasted_iota(jnp.int32, (8, LANES), 0)
    lane = lax.broadcasted_iota(jnp.int32, (8, LANES), 1)
    turned = pltpu.roll(keys[0], 7, 0)
    following = jnp.where(sub == 7, pltpu.roll(turned, LANES - 1, 1), turned)
    following = jnp.where((sub == 7) & (lane == LANES - 1), -1, following)
    high_label = lax.broadcasted_iota(jnp.int32, (table, LANES), 0)
    low_label = lax.broadcasted_iota(jnp.int32, (LANES, LANES), 0)
    found = jnp.zeros((4 * table, LANES), jnp.float32)
    for t in range(count):
        last = keys[t] != (keys[t + 1] if t + 1 < count else following)
        high = jnp.where(last, keys[t] // LANES, -1)
        low = keys[t] % LANES
        first = values[t].astype(jnp.bfloat16).astype(jnp.float32)
        rest = values[t] - first
        second = rest.astype(jnp.bfloat16).astype(jnp.float32)
        third = rest - second
        left, right = [], []
        for r in range(8):
            member = high[r:r + 1] == high_label
            pieces = [jnp.where(member, x[r:r + 1], 0.0) for x in (first, second, third)]
            pieces.append(jnp.where(member, 1.0, 0.0))
            left.append(jnp.concatenate(pieces, axis=0).astype(jnp.bfloat16))
            right.append(jnp.where(low[r:r + 1] == low_label, 1.0, 0.0).astype(jnp.bfloat16))
        found = found + lax.dot_general(jnp.concatenate(left, axis=1), jnp.concatenate(right, axis=1),
                                        (((1,), (1,)), ((), ())), preferred_element_type=jnp.float32)
    top = (found[0:table] + found[table:2 * table]) + found[2 * table:3 * table]
    return jnp.where(found[3 * table:] > 0.5, top, floor_value)


def plan(chips):
    if chips == 4:
        order = [[3, 1, 2, 0], [2, 3, 0, 1], [1, 0, 3, 2], [0, 2, 1, 3]]
        target = [[1, 1, 2], [2, 3, 0], [1, 0, 3], [2, 2, 1]]
        merged = [[1, 0, 0], [0, 0, 0], [0, 0, 0], [1, 0, 0]]
        return order, target, merged, {1: (1, 2)}, {(0, 3), (3, 0)}
    order = [sorted((d for d in range(chips) if d != c), key=lambda d: -abs(d - c)) + [c] for c in range(chips)]
    target = [o[:-1] for o in order]
    merged = [[0] * (chips - 1) for _ in range(chips)]
    return order, target, merged, {}, set()


def pick(table, chip):
    value = table[0]
    for c in range(1, len(table)):
        if table[c] != table[c - 1]:
            value = value + jnp.where(chip >= c, table[c] - table[c - 1], 0)
    return value


def kernel(groups, whole_count, lw_hbm, bins_hbm, states_hbm, cum_ref, means_ref, weights_ref,
           lw_ref, bins_ref, held, ext, lo_b, hi_b, part_b, w_b, top_tab, blocks,
           pair_send, pair_recv, pair_send_s, pair_recv_s, send, recv, send_s, recv_s, fac, own_s,
           stat_send, stat_recv, load_sem, pair_ss, pair_rs, chip_ss, chip_rs, stat_ss, stat_rs):
    state = held.shape[0]
    count = held.shape[1]
    rows = count // LANES
    owned = BINS // groups
    both = 2 * owned
    width = min(256, owned)
    split = both // width
    half = split // 2
    chunks = owned // LANES
    per = width // LANES
    chips = groups // 2
    order, target, merged, merging, skipped = plan(chips)
    me = lax.axis_index("dom")
    chip, core = me // 2, me % 2
    partner = chip * 2 + (1 - core)

    loads = [pltpu.make_async_copy(src, dst, load_sem.at[i]) for i, (src, dst) in enumerate(
        ((lw_hbm, lw_ref), (bins_hbm, bins_ref), (states_hbm, held)))]
    for load in loads:
        load.start()
    barrier = pltpu.get_barrier_semaphore()
    for k in range(1, groups):
        pl.semaphore_signal(barrier, inc=1, device_id={"dom": lax.rem(me + k, groups)},
                            device_id_type=pl.DeviceIdType.MESH)
    loads[0].wait()
    loads[1].wait()

    lw = lw_ref[...]
    bins = bins_ref[...]
    spread_rows(lo_b, (bins % width).astype(jnp.float32))
    spread_rows(hi_b, (bins // both).astype(jnp.float32))
    spread_rows(part_b, ((bins % both) // width).astype(jnp.float32))
    tops = local_tops(lw, bins)
    low, high = bins % LANES, bins // LANES
    own_top = jnp.zeros(lw.shape, jnp.float32)
    for t in range(BINS // LANES):
        picked = jnp.take_along_axis(jnp.broadcast_to(tops[t:t + 1], lw.shape), low, axis=1)
        own_top = jnp.where(high == t, picked, own_top)
        top_tab[t] = jnp.broadcast_to(tops[t:t + 1], (8, LANES))
    spread_rows(w_b, jnp.exp(lw - own_top))
    loads[2].wait()

    zero = jnp.zeros((), jnp.bfloat16)
    one_label = lax.broadcasted_iota(jnp.int32, (EXTRA, LANES), 0) // (EXTRA // split)
    one_label = one_label.astype(jnp.float32).astype(jnp.bfloat16)

    def mask_states(r, carry):
        part = part_b[pl.ds(pl.multiple_of(r * 16, 16), 16), :]
        cols = pl.ds(pl.multiple_of(r * LANES, LANES), LANES)
        tile = held[:, cols]
        part_all = jnp.concatenate([part] * (state // 16), axis=0)
        for q in range(split):
            ext[q * state:(q + 1) * state, cols] = jnp.where(part_all == jnp.bfloat16(q), tile, zero)
        ext[split * state:split * state + EXTRA, cols] = jnp.where(part == one_label, jnp.bfloat16(1), zero)
        return carry

    lax.fori_loop(0, rows, mask_states, 0)
    pl.semaphore_wait(barrier, groups - 1)

    depth = min(64, rows) if chips <= 4 else 16
    label = lax.broadcasted_iota(jnp.int32, (width, LANES), 0).astype(jnp.float32).astype(jnp.bfloat16)

    def accumulate(dest, out, c):
        tile = jnp.asarray(dest).astype(jnp.float32).astype(jnp.bfloat16)
        pieces = []
        for j in range(depth):
            at = pl.ds(pl.multiple_of((c * depth + j) * 16, 16), 16)
            w = jnp.where(hi_b[at, :] == tile, w_b[at, :], zero)
            lo = lo_b[at, :]
            w_all = jnp.concatenate([w] * (width // 16), axis=0)
            lo_all = jnp.concatenate([lo] * (width // 16), axis=0)
            pieces.append(jnp.where(lo_all == label, w_all, zero))
        spread = jnp.concatenate(pieces, axis=1)
        cols = pl.ds(pl.multiple_of(c * depth * LANES, LANES), depth * LANES)
        out[...] += lax.dot_general(ext[:, cols], spread, (((1,), (1,)), ((), ())),
                                    preferred_element_type=jnp.float32)

    def remote(src, dst, ss, rs, chip_to, core_to):
        return pltpu.make_async_remote_copy(src, dst, ss, rs, device_id={"dom": chip_to * 2 + core_to},
                                            device_id_type=pl.DeviceIdType.MESH)

    def sums_of(found, which, j):
        at = pl.multiple_of((which * half + j // per) * state, state)
        return found[pl.ds(at, state), (j % per) * LANES:(j % per + 1) * LANES]

    def mass_of(found, which, j):
        lanes = slice((j % per) * LANES, (j % per + 1) * LANES)
        at = split * state + (j // per) * (EXTRA // split)
        first = found[at:at + 1, lanes]
        at = at + half * (EXTRA // split)
        return jnp.where(which == 0, first, found[at:at + 1, lanes])

    def stats_of(found, dest, which):
        mass = [mass_of(found, which, j) for j in range(chunks)]
        top = [top_tab[(dest * 2 + which) * chunks + j][0:1] for j in range(chunks)]
        pad = [jnp.zeros((4 - chunks, LANES), jnp.float32)] if chunks < 4 else []
        return jnp.concatenate(mass + pad, axis=0), jnp.concatenate(top + pad, axis=0)

    def pair_copies(s):
        return (remote(pair_send_s.at[s], pair_recv_s.at[s], pair_ss.at[0, s], pair_rs.at[0, s], chip, 1 - core),
                remote(pair_send.at[s], pair_recv.at[s], pair_ss.at[1, s], pair_rs.at[1, s], chip, 1 - core))

    def give(s, dest):
        found = blocks.at[s % 2]
        mass, top = stats_of(found, dest, 1 - core)
        pair_send_s[s, 0:4] = mass
        pair_send_s[s, 4:8] = top
        for j in range(chunks):
            pair_send[s, j * state:(j + 1) * state] = sums_of(found, 1 - core, j)
        for copy in pair_copies(s):
            copy.start()

    def incoming(slot):
        return (remote(send_s.at[0], recv_s.at[slot], chip_ss.at[0, 0], chip_rs.at[0, slot], chip, 1 - core),
                remote(send.at[0], recv.at[slot], chip_ss.at[1, 0], chip_rs.at[1, slot], chip, 1 - core))

    def outgoing(s):
        to = pick([t[s] for t in target], chip)
        slot = chip + pick([m[s] for m in merged], chip) * (chips - chip)
        return (remote(send_s.at[s], recv_s.at[slot], chip_ss.at[0, s], chip_rs.at[0, slot], to, core),
                remote(send.at[s], recv.at[slot], chip_ss.at[1, s], chip_rs.at[1, slot], to, core))

    def handle(s, dest):
        found = blocks.at[s % 2]
        for copy in pair_copies(s):
            copy.wait_recv()
        mass, top = stats_of(found, dest, core)
        theirs = pair_recv_s[s, 4:8]
        most = jnp.maximum(top, theirs)
        by_mine, by_theirs = jnp.exp(top - most), jnp.exp(theirs - most)
        send_s[s, 0:4] = mass * by_mine + pair_recv_s[s, 0:4] * by_theirs
        send_s[s, 4:8] = most
        for j in range(chunks):
            at = slice(j * state, (j + 1) * state)
            send[s, at] = sums_of(found, core, j) * by_mine[j:j + 1] + pair_recv[s, at] * by_theirs[j:j + 1]
        if s in merging:
            first, last = merging[s]

            @pl.when((chip >= first) & (chip <= last))
            def _():
                for copy in incoming(chips):
                    copy.wait_recv()
                mine, theirs = send_s[s, 4:8], recv_s[chips, 4:8]
                most = jnp.maximum(mine, theirs)
                by_mine, by_theirs = jnp.exp(mine - most), jnp.exp(theirs - most)
                send_s[s, 0:4] = send_s[s, 0:4] * by_mine + recv_s[chips, 0:4] * by_theirs
                send_s[s, 4:8] = most
                for j in range(chunks):
                    at = slice(j * state, (j + 1) * state)
                    send[s, at] = send[s, at] * by_mine[j:j + 1] + recv[chips, at] * by_theirs[j:j + 1]
        if s < chips - 1:
            for copy in outgoing(s):
                copy.start()

    dests = [pick([o[s] for o in order], chip) for s in range(chips)]
    for s in range(chips):
        found = blocks.at[s % 2]
        found[...] = jnp.zeros(found.shape, jnp.float32)

        def step(c, carry, s=s, found=found):
            accumulate(dests[s], found, c)
            if s:
                @pl.when(c == 0)
                def _():
                    handle(s - 1, dests[s - 1])
            return carry

        lax.fori_loop(0, rows // depth, step, 0)
        give(s, dests[s])

    last = chips - 1

    def valid(sender):
        ok = chip != sender
        for owner, other in skipped:
            if other == sender:
                ok = ok & (chip != owner)
        return ok

    handle(last, dests[last])
    for c in range(chips):
        @pl.when(valid(c))
        def _(c=c):
            incoming(c)[0].wait_recv()

        @pl.when(jnp.logical_not(valid(c)))
        def _(c=c):
            recv_s[c, 0:4] = jnp.zeros((4, LANES), jnp.float32)
            recv_s[c, 4:8] = jnp.full((4, LANES), floor_value, jnp.float32)

    own_top = send_s[last, 4:8]
    bin_top = own_top
    for c in range(chips):
        bin_top = jnp.maximum(bin_top, recv_s[c, 4:8])
    by_own = jnp.exp(own_top - bin_top)
    mass = send_s[last, 0:4] * by_own
    for c in range(chips):
        by = jnp.exp(recv_s[c, 4:8] - bin_top)
        fac[c] = by
        mass = mass + recv_s[c, 0:4] * by
    real = lax.broadcasted_iota(jnp.int32, (4, LANES), 0) < chunks
    block_top = jnp.max(jnp.max(jnp.where(real, bin_top, floor_value), axis=1, keepdims=True), axis=0, keepdims=True)
    share = jnp.where(real, mass * jnp.exp(bin_top - block_top), 0.0)
    block_mass = jnp.sum(jnp.sum(share, axis=1, keepdims=True), axis=0, keepdims=True)
    stat_send[0:4, :] = jnp.broadcast_to(block_top, (4, LANES))
    stat_send[4:8, :] = jnp.broadcast_to(block_mass, (4, LANES))
    stat_copies = []
    for k in range(1, groups):
        copy = pltpu.make_async_remote_copy(
            stat_send, stat_recv.at[k - 1], stat_ss.at[k - 1], stat_rs.at[k - 1],
            device_id={"dom": lax.rem(me + k, groups)}, device_id_type=pl.DeviceIdType.MESH)
        copy.start()
        stat_copies.append(copy)
    for j in range(chunks):
        at = slice(j * state, (j + 1) * state)
        send[last, at] = send[last, at] * by_own[j:j + 1]
    run = share
    position = lax.broadcasted_iota(jnp.int32, run.shape, 1)
    hop = 1
    while hop < LANES:
        run = run + jnp.where(position >= hop, pltpu.roll(run, hop, 1), 0.0)
        hop *= 2
    sums = [jnp.sum(share[j:j + 1], axis=1, keepdims=True) for j in range(chunks)]
    base = jnp.zeros((1, 1), jnp.float32)
    runs = []
    for j in range(chunks):
        runs.append(run[j:j + 1] + base)
        base = base + sums[j]
    for copy in stat_copies:
        copy.wait_recv()
    top = block_top
    for k in range(groups - 1):
        top = jnp.maximum(top, stat_recv[k, 0:1, 0:1])
    scale = jnp.exp(block_top - top)
    total = block_mass * scale
    before = jnp.zeros_like(total)
    for k in range(groups - 1):
        theirs = stat_recv[k, 4:5, 0:1] * jnp.exp(stat_recv[k, 0:1, 0:1] - top)
        total = total + theirs
        before = before + jnp.where(me >= k + 1, theirs, 0.0)
    cum_ref[...] = (before + jnp.concatenate(runs, axis=1) * scale) / total
    weights_ref[...] = whole_count * jnp.exp(lw_ref[...] - top) / total
    for c in range(chips):
        @pl.when(valid(c))
        def _(c=c):
            incoming(c)[1].wait_recv()
            for j in range(chunks):
                at = slice(j * state, (j + 1) * state)
                send[last, at] = send[last, at] + recv[c, at] * fac[c, j:j + 1]
    for j in range(chunks):
        means_ref[:, j * LANES:(j + 1) * LANES] = (send[last, j * state:(j + 1) * state]
                                                   / jnp.maximum(mass[j:j + 1], 1.0))
    for s in range(chips):
        for copy in pair_copies(s):
            copy.wait_send()
    for s in range(last):
        for copy in outgoing(s):
            copy.wait_send()
    for copy in stat_copies:
        copy.wait_send()


def body(log_weights, bins, states):
    groups = lax.axis_size("dom")
    owned = BINS // groups
    chips = groups // 2
    state, count = states.shape
    rows = count // LANES
    width = min(256, owned)
    split = 2 * owned // width
    chunks = owned // LANES
    vmem = pl.BlockSpec(memory_space=pltpu.VMEM)
    hbm = pl.BlockSpec(memory_space=pltpu.HBM)

    def sums(slots):
        return pltpu.VMEM((slots, chunks * state, LANES), jnp.float32)

    def stats(slots):
        return pltpu.VMEM((slots, 8, LANES), jnp.float32)

    cumulative, bin_means, weights = pl.pallas_call(
        functools.partial(kernel, groups, float(count * groups)),
        out_shape=(jax.ShapeDtypeStruct((1, owned), jnp.float32),
                   jax.ShapeDtypeStruct((state, owned), jnp.float32),
                   jax.ShapeDtypeStruct((rows, LANES), jnp.float32)),
        in_specs=[hbm, hbm, hbm],
        out_specs=(vmem, vmem, vmem),
        scratch_shapes=[
            pltpu.VMEM((rows, LANES), jnp.float32),
            pltpu.VMEM((rows, LANES), jnp.int32),
            pltpu.VMEM((state, count), jnp.bfloat16),
            pltpu.VMEM((split * state + EXTRA, count), jnp.bfloat16),
            pltpu.VMEM((rows * 16, LANES), jnp.bfloat16),
            pltpu.VMEM((rows * 16, LANES), jnp.bfloat16),
            pltpu.VMEM((rows * 16, LANES), jnp.bfloat16),
            pltpu.VMEM((rows * 16, LANES), jnp.bfloat16),
            pltpu.VMEM((BINS // LANES, 8, LANES), jnp.float32),
            pltpu.VMEM((2, split * state + EXTRA, width), jnp.float32),
            sums(chips), sums(chips), stats(chips), stats(chips),
            sums(chips), sums(chips + 1), stats(chips), stats(chips + 1),
            pltpu.VMEM((chips, 4, LANES), jnp.float32),
            pltpu.VMEM((8, LANES), jnp.float32),
            pltpu.VMEM((8, LANES), jnp.float32),
            pltpu.VMEM((groups - 1, 8, LANES), jnp.float32),
            pltpu.SemaphoreType.DMA((3,)),
            pltpu.SemaphoreType.DMA((2, chips)),
            pltpu.SemaphoreType.DMA((2, chips)),
            pltpu.SemaphoreType.DMA((2, chips)),
            pltpu.SemaphoreType.DMA((2, chips + 1)),
            pltpu.SemaphoreType.DMA((groups - 1,)),
            pltpu.SemaphoreType.DMA((groups - 1,)),
        ],
        compiler_params=pltpu.CompilerParams(
            collective_id=0, has_side_effects=True, vmem_limit_bytes=48 * 1024 * 1024),
    )(log_weights.reshape(rows, LANES), bins.reshape(rows, LANES), states)
    return cumulative.reshape(owned), bin_means, weights.reshape(count)


def solution(mesh):
    placed = (P(("filt", "dom")), P(("filt", "dom")), P(None, ("filt", "dom")))
    return jax.shard_map(
        body,
        mesh=mesh,
        in_specs=placed,
        out_specs=(P(("filt", "dom")), P(None, ("filt", "dom")), P(("filt", "dom"))),
        check_vma=False,
    )
```

```python
import functools

import jax
import jax.numpy as jnp
from jax import lax
from jax.experimental import pallas as pl
from jax.experimental.pallas import tpu as pltpu
from jax.sharding import PartitionSpec as P

BINS = 4096
LANES = 128
EXTRA = 16
LEVEL_BITS = 20
LEVELS = 1 << LEVEL_BITS
LEAST = -20.0
PER_UNIT = (LEVELS - 3) / 270.0

floor_value = -10000.0


def spread_rows(ref, values):
    for r in range(values.shape[0]):
        ref[16 * r:16 * r + 16, :] = jnp.broadcast_to(values[r:r + 1, :], (16, LANES)).astype(ref.dtype)


def sort_keys(keys):
    tile_bits = len(keys).bit_length() - 1
    bits = tile_bits + 10
    sub = lax.broadcasted_iota(jnp.int32, (8, LANES), 0)
    lane = lax.broadcasted_iota(jnp.int32, (8, LANES), 1)

    def mask_of(bit):
        if bit < tile_bits + 3:
            return (sub >> (bit - tile_bits)) & 1
        return (lane >> (bit - tile_bits - 3)) & 1

    def turned(size):
        if size >= bits:
            return None
        if size < tile_bits:
            return [-((t >> size) & 1) for t in range(len(keys))]
        return -mask_of(size)

    def flip(now, then):
        for t in range(len(keys)):
            a = now[t] if isinstance(now, list) else now
            b = then[t] if isinstance(then, list) else then
            if a is None:
                a = 0
            if b is None:
                b = 0
            if isinstance(a, int) and isinstance(b, int):
                if a != b:
                    keys[t] = ~keys[t]
                continue
            keys[t] = keys[t] ^ (a ^ b)

    before = None
    for size in range(1, bits + 1):
        down = turned(size)
        flip(before, down)
        before = down
        for bit in range(size - 1, -1, -1):
            if bit < tile_bits:
                for t in range(len(keys)):
                    o = t | (1 << bit)
                    if o != t:
                        keys[t], keys[o] = jnp.minimum(keys[t], keys[o]), jnp.maximum(keys[t], keys[o])
                continue
            upper = mask_of(bit) != 0
            if bit < tile_bits + 3:
                index, axis = sub ^ (1 << (bit - tile_bits)), 0
            else:
                index, axis = lane ^ (1 << (bit - tile_bits - 3)), 1
            for t in range(len(keys)):
                k = jnp.take_along_axis(keys[t], index, axis=axis)
                keys[t] = jnp.where(upper, jnp.maximum(keys[t], k), jnp.minimum(keys[t], k))
    return keys


def local_tops(lw, bins):
    count = lw.shape[0] // 8
    table = BINS // LANES
    level = jnp.clip((lw - LEAST) * PER_UNIT + 1.5, 1.0, float(LEVELS - 1)).astype(jnp.int32)
    packed = (bins - BINS // 2) * LEVELS + level
    keys = sort_keys([packed[8 * t:8 * t + 8] for t in range(count)])
    sub = lax.broadcasted_iota(jnp.int32, (8, LANES), 0)
    lane = lax.broadcasted_iota(jnp.int32, (8, LANES), 1)
    places = [(k >> LEVEL_BITS) + BINS // 2 for k in keys]
    turned = pltpu.roll(places[0], 7, 0)
    following = jnp.where(sub == 7, pltpu.roll(turned, LANES - 1, 1), turned)
    following = jnp.where((sub == 7) & (lane == LANES - 1), -1, following)
    high_label = lax.broadcasted_iota(jnp.int32, (table, LANES), 0).astype(jnp.float32).astype(jnp.bfloat16)
    low_label = lax.broadcasted_iota(jnp.int32, (LANES, LANES), 0).astype(jnp.float32).astype(jnp.bfloat16)
    zero, one = jnp.zeros((), jnp.bfloat16), jnp.ones((), jnp.bfloat16)
    found = jnp.zeros((3 * table, LANES), jnp.float32)

    def row(x, r):
        return jnp.broadcast_to(x[r:r + 1], (16, LANES)).astype(jnp.bfloat16)

    for t in range(count):
        last = places[t] != (places[t + 1] if t + 1 < count else following)
        high = jnp.where(last, places[t] // LANES, -1).astype(jnp.float32)
        low = (places[t] % LANES).astype(jnp.float32)
        size = keys[t] & (LEVELS - 1)
        parts = [(size >> 12).astype(jnp.float32), ((size >> 4) & 255).astype(jnp.float32),
                 (size & 15).astype(jnp.float32)]
        left, right = [], []
        for r in range(8):
            member = jnp.concatenate([row(high, r)] * (table // 16), axis=0) == high_label
            left.append(jnp.concatenate(
                [jnp.where(member, jnp.concatenate([row(x, r)] * (table // 16), axis=0), zero) for x in parts], axis=0))
            right.append(jnp.where(jnp.concatenate([row(low, r)] * (LANES // 16), axis=0) == low_label, one, zero))
        found = found + lax.dot_general(jnp.concatenate(left, axis=1), jnp.concatenate(right, axis=1),
                                        (((1,), (1,)), ((), ())), preferred_element_type=jnp.float32)
    top = (found[0:table] * 4096.0 + found[table:2 * table] * 16.0) + found[2 * table:3 * table]
    return jnp.where(top > 0.5, (top - 1.0) * (1.0 / PER_UNIT) + LEAST, floor_value)


def plan(chips):
    if chips == 4:
        order = [[3, 1, 2, 0], [2, 3, 0, 1], [1, 0, 3, 2], [0, 2, 1, 3]]
        target = [[1, 1, 2], [2, 3, 0], [1, 0, 3], [2, 2, 1]]
        merged = [[1, 0, 0], [0, 0, 0], [0, 0, 0], [1, 0, 0]]
        return order, target, merged, {1: (1, 2)}, {(0, 3), (3, 0)}
    order = [sorted((d for d in range(chips) if d != c), key=lambda d: -abs(d - c)) + [c] for c in range(chips)]
    target = [o[:-1] for o in order]
    merged = [[0] * (chips - 1) for _ in range(chips)]
    return order, target, merged, {}, set()


def pick(table, chip):
    value = table[0]
    for c in range(1, len(table)):
        if table[c] != table[c - 1]:
            value = value + jnp.where(chip >= c, table[c] - table[c - 1], 0)
    return value


def kernel(groups, whole_count, lw_ref, bins_ref, states_hbm, cum_ref, means_ref, weights_ref,
           held, ext, lo_b, hi_b, part_b, w_b, top_tab, blocks,
           pair_send, pair_recv, pair_send_s, pair_recv_s, send, recv, send_s, recv_s, fac, own_s,
           stat_send, stat_recv, load_sem, pair_ss, pair_rs, chip_ss, chip_rs, stat_ss, stat_rs):
    state = held.shape[0]
    count = held.shape[1]
    rows = count // LANES
    owned = BINS // groups
    both = 2 * owned
    width = min(256, owned)
    split = both // width
    half = split // 2
    chunks = owned // LANES
    per = width // LANES
    chips = groups // 2
    order, target, merged, merging, skipped = plan(chips)
    me = lax.axis_index("dom")
    chip, core = me // 2, me % 2
    partner = chip * 2 + (1 - core)

    load = pltpu.make_async_copy(states_hbm, held, load_sem)
    load.start()
    barrier = pltpu.get_barrier_semaphore()
    for k in range(1, groups):
        pl.semaphore_signal(barrier, inc=1, device_id={"dom": lax.rem(me + k, groups)},
                            device_id_type=pl.DeviceIdType.MESH)

    lw = lw_ref[...]
    bins = bins_ref[...]
    spread_rows(lo_b, (bins % width).astype(jnp.float32))
    spread_rows(hi_b, (bins // both).astype(jnp.float32))
    spread_rows(part_b, ((bins % both) // width).astype(jnp.float32))
    tops = local_tops(lw, bins)
    low, high = bins % LANES, bins // LANES
    own_top = jnp.zeros(lw.shape, jnp.float32)
    for t in range(BINS // LANES):
        picked = jnp.take_along_axis(jnp.broadcast_to(tops[t:t + 1], lw.shape), low, axis=1)
        own_top = jnp.where(high == t, picked, own_top)
        top_tab[t] = jnp.broadcast_to(tops[t:t + 1], (8, LANES))
    spread_rows(w_b, jnp.exp(lw - own_top))
    load.wait()

    zero = jnp.zeros((), jnp.bfloat16)
    one_label = lax.broadcasted_iota(jnp.int32, (EXTRA, LANES), 0) // (EXTRA // split)
    one_label = one_label.astype(jnp.float32).astype(jnp.bfloat16)

    def mask_states(r, carry):
        part = part_b[pl.ds(pl.multiple_of(r * 16, 16), 16), :]
        cols = pl.ds(pl.multiple_of(r * LANES, LANES), LANES)
        tile = held[:, cols]
        part_all = jnp.concatenate([part] * (state // 16), axis=0)
        for q in range(split):
            ext[q * state:(q + 1) * state, cols] = jnp.where(part_all == jnp.bfloat16(q), tile, zero)
        ext[split * state:split * state + EXTRA, cols] = jnp.where(part == one_label, jnp.bfloat16(1), zero)
        return carry

    lax.fori_loop(0, rows, mask_states, 0)
    pl.semaphore_wait(barrier, groups - 1)

    depth = min(64, rows) if chips <= 4 else 16
    label = lax.broadcasted_iota(jnp.int32, (width, LANES), 0).astype(jnp.float32).astype(jnp.bfloat16)

    def accumulate(dest, out, c):
        tile = jnp.asarray(dest).astype(jnp.float32).astype(jnp.bfloat16)
        pieces = []
        for j in range(depth):
            at = pl.ds(pl.multiple_of((c * depth + j) * 16, 16), 16)
            w = jnp.where(hi_b[at, :] == tile, w_b[at, :], zero)
            lo = lo_b[at, :]
            w_all = jnp.concatenate([w] * (width // 16), axis=0)
            lo_all = jnp.concatenate([lo] * (width // 16), axis=0)
            pieces.append(jnp.where(lo_all == label, w_all, zero))
        spread = jnp.concatenate(pieces, axis=1)
        cols = pl.ds(pl.multiple_of(c * depth * LANES, LANES), depth * LANES)
        out[...] += lax.dot_general(ext[:, cols], spread, (((1,), (1,)), ((), ())),
                                    preferred_element_type=jnp.float32)

    def remote(src, dst, ss, rs, chip_to, core_to):
        return pltpu.make_async_remote_copy(src, dst, ss, rs, device_id={"dom": chip_to * 2 + core_to},
                                            device_id_type=pl.DeviceIdType.MESH)

    def sums_of(found, which, j):
        at = pl.multiple_of((which * half + j // per) * state, state)
        return found[pl.ds(at, state), (j % per) * LANES:(j % per + 1) * LANES]

    def mass_of(found, which, j):
        lanes = slice((j % per) * LANES, (j % per + 1) * LANES)
        at = split * state + (j // per) * (EXTRA // split)
        first = found[at:at + 1, lanes]
        at = at + half * (EXTRA // split)
        return jnp.where(which == 0, first, found[at:at + 1, lanes])

    def stats_of(found, dest, which):
        mass = [mass_of(found, which, j) for j in range(chunks)]
        top = [top_tab[(dest * 2 + which) * chunks + j][0:1] for j in range(chunks)]
        pad = [jnp.zeros((4 - chunks, LANES), jnp.float32)] if chunks < 4 else []
        return jnp.concatenate(mass + pad, axis=0), jnp.concatenate(top + pad, axis=0)

    def pair_copies(s):
        return (remote(pair_send_s.at[s], pair_recv_s.at[s], pair_ss.at[0, s], pair_rs.at[0, s], chip, 1 - core),
                remote(pair_send.at[s], pair_recv.at[s], pair_ss.at[1, s], pair_rs.at[1, s], chip, 1 - core))

    def give(s, dest):
        found = blocks.at[s % 2]
        mass, top = stats_of(found, dest, 1 - core)
        pair_send_s[s, 0:4] = mass
        pair_send_s[s, 4:8] = top
        for j in range(chunks):
            pair_send[s, j * state:(j + 1) * state] = sums_of(found, 1 - core, j)
        for copy in pair_copies(s):
            copy.start()

    def incoming(slot):
        return (remote(send_s.at[0], recv_s.at[slot], chip_ss.at[0, 0], chip_rs.at[0, slot], chip, 1 - core),
                remote(send.at[0], recv.at[slot], chip_ss.at[1, 0], chip_rs.at[1, slot], chip, 1 - core))

    def outgoing(s):
        to = pick([t[s] for t in target], chip)
        slot = chip + pick([m[s] for m in merged], chip) * (chips - chip)
        return (remote(send_s.at[s], recv_s.at[slot], chip_ss.at[0, s], chip_rs.at[0, slot], to, core),
                remote(send.at[s], recv.at[slot], chip_ss.at[1, s], chip_rs.at[1, slot], to, core))

    def handle(s, dest):
        found = blocks.at[s % 2]
        for copy in pair_copies(s):
            copy.wait_recv()
        mass, top = stats_of(found, dest, core)
        theirs = pair_recv_s[s, 4:8]
        most = jnp.maximum(top, theirs)
        by_mine, by_theirs = jnp.exp(top - most), jnp.exp(theirs - most)
        send_s[s, 0:4] = mass * by_mine + pair_recv_s[s, 0:4] * by_theirs
        send_s[s, 4:8] = most
        for j in range(chunks):
            at = slice(j * state, (j + 1) * state)
            send[s, at] = sums_of(found, core, j) * by_mine[j:j + 1] + pair_recv[s, at] * by_theirs[j:j + 1]
        if s in merging:
            first, last = merging[s]

            @pl.when((chip >= first) & (chip <= last))
            def _():
                for copy in incoming(chips):
                    copy.wait_recv()
                mine, theirs = send_s[s, 4:8], recv_s[chips, 4:8]
                most = jnp.maximum(mine, theirs)
                by_mine, by_theirs = jnp.exp(mine - most), jnp.exp(theirs - most)
                send_s[s, 0:4] = send_s[s, 0:4] * by_mine + recv_s[chips, 0:4] * by_theirs
                send_s[s, 4:8] = most
                for j in range(chunks):
                    at = slice(j * state, (j + 1) * state)
                    send[s, at] = send[s, at] * by_mine[j:j + 1] + recv[chips, at] * by_theirs[j:j + 1]
        if s < chips - 1:
            for copy in outgoing(s):
                copy.start()

    dests = [pick([o[s] for o in order], chip) for s in range(chips)]
    for s in range(chips):
        found = blocks.at[s % 2]
        found[...] = jnp.zeros(found.shape, jnp.float32)

        def step(c, carry, s=s, found=found):
            accumulate(dests[s], found, c)
            if s:
                @pl.when(c == 0)
                def _():
                    handle(s - 1, dests[s - 1])
            return carry

        lax.fori_loop(0, rows // depth, step, 0)
        give(s, dests[s])

    last = chips - 1

    def valid(sender):
        ok = chip != sender
        for owner, other in skipped:
            if other == sender:
                ok = ok & (chip != owner)
        return ok

    handle(last, dests[last])
    for c in range(chips):
        @pl.when(valid(c))
        def _(c=c):
            incoming(c)[0].wait_recv()

        @pl.when(jnp.logical_not(valid(c)))
        def _(c=c):
            recv_s[c, 0:4] = jnp.zeros((4, LANES), jnp.float32)
            recv_s[c, 4:8] = jnp.full((4, LANES), floor_value, jnp.float32)

    own_top = send_s[last, 4:8]
    bin_top = own_top
    for c in range(chips):
        bin_top = jnp.maximum(bin_top, recv_s[c, 4:8])
    by_own = jnp.exp(own_top - bin_top)
    mass = send_s[last, 0:4] * by_own
    for c in range(chips):
        by = jnp.exp(recv_s[c, 4:8] - bin_top)
        fac[c] = by
        mass = mass + recv_s[c, 0:4] * by
    real = lax.broadcasted_iota(jnp.int32, (4, LANES), 0) < chunks
    block_top = jnp.max(jnp.max(jnp.where(real, bin_top, floor_value), axis=1, keepdims=True), axis=0, keepdims=True)
    share = jnp.where(real, mass * jnp.exp(bin_top - block_top), 0.0)
    block_mass = jnp.sum(jnp.sum(share, axis=1, keepdims=True), axis=0, keepdims=True)
    stat_send[0:4, :] = jnp.broadcast_to(block_top, (4, LANES))
    stat_send[4:8, :] = jnp.broadcast_to(block_mass, (4, LANES))
    stat_copies = []
    for k in range(1, groups):
        copy = pltpu.make_async_remote_copy(
            stat_send, stat_recv.at[k - 1], stat_ss.at[k - 1], stat_rs.at[k - 1],
            device_id={"dom": lax.rem(me + k, groups)}, device_id_type=pl.DeviceIdType.MESH)
        copy.start()
        stat_copies.append(copy)
    for j in range(chunks):
        at = slice(j * state, (j + 1) * state)
        send[last, at] = send[last, at] * by_own[j:j + 1]
    run = share
    position = lax.broadcasted_iota(jnp.int32, run.shape, 1)
    hop = 1
    while hop < LANES:
        run = run + jnp.where(position >= hop, pltpu.roll(run, hop, 1), 0.0)
        hop *= 2
    sums = [jnp.sum(share[j:j + 1], axis=1, keepdims=True) for j in range(chunks)]
    base = jnp.zeros((1, 1), jnp.float32)
    runs = []
    for j in range(chunks):
        runs.append(run[j:j + 1] + base)
        base = base + sums[j]
    for copy in stat_copies:
        copy.wait_recv()
    top = block_top
    for k in range(groups - 1):
        top = jnp.maximum(top, stat_recv[k, 0:1, 0:1])
    scale = jnp.exp(block_top - top)
    total = block_mass * scale
    before = jnp.zeros_like(total)
    for k in range(groups - 1):
        theirs = stat_recv[k, 4:5, 0:1] * jnp.exp(stat_recv[k, 0:1, 0:1] - top)
        total = total + theirs
        before = before + jnp.where(me >= k + 1, theirs, 0.0)
    cum_ref[...] = (before + jnp.concatenate(runs, axis=1) * scale) / total
    weights_ref[...] = whole_count * jnp.exp(lw_ref[...] - top) / total
    for c in range(chips):
        @pl.when(valid(c))
        def _(c=c):
            incoming(c)[1].wait_recv()
            for j in range(chunks):
                at = slice(j * state, (j + 1) * state)
                send[last, at] = send[last, at] + recv[c, at] * fac[c, j:j + 1]
    for j in range(chunks):
        means_ref[:, j * LANES:(j + 1) * LANES] = (send[last, j * state:(j + 1) * state]
                                                   / jnp.maximum(mass[j:j + 1], 1.0))
    for s in range(chips):
        for copy in pair_copies(s):
            copy.wait_send()
    for s in range(last):
        for copy in outgoing(s):
            copy.wait_send()
    for copy in stat_copies:
        copy.wait_send()


def drain(*refs):
    sources, results, sems = refs[0:3], refs[3:6], refs[6]
    copies = [pltpu.make_async_copy(sources[i], results[i], sems.at[i]) for i in range(3)]
    for copy in copies:
        copy.start()
    for copy in copies:
        copy.wait()


def body(log_weights, bins, states):
    groups = lax.axis_size("dom")
    owned = BINS // groups
    chips = groups // 2
    state, count = states.shape
    rows = count // LANES
    width = min(256, owned)
    split = 2 * owned // width
    chunks = owned // LANES
    vmem = pl.BlockSpec(memory_space=pltpu.VMEM)
    hbm = pl.BlockSpec(memory_space=pltpu.HBM)

    def sums(slots):
        return pltpu.VMEM((slots, chunks * state, LANES), jnp.float32)

    def stats(slots):
        return pltpu.VMEM((slots, 8, LANES), jnp.float32)

    shapes = (jax.ShapeDtypeStruct((1, owned), jnp.float32),
              jax.ShapeDtypeStruct((state, owned), jnp.float32),
              jax.ShapeDtypeStruct((rows, LANES), jnp.float32))
    found = pl.pallas_call(
        functools.partial(kernel, groups, float(count * groups)),
        out_shape=shapes,
        in_specs=[vmem, vmem, hbm],
        out_specs=(vmem, vmem, vmem),
        scratch_shapes=[
            pltpu.VMEM((state, count), jnp.bfloat16),
            pltpu.VMEM((split * state + EXTRA, count), jnp.bfloat16),
            pltpu.VMEM((rows * 16, LANES), jnp.bfloat16),
            pltpu.VMEM((rows * 16, LANES), jnp.bfloat16),
            pltpu.VMEM((rows * 16, LANES), jnp.bfloat16),
            pltpu.VMEM((rows * 16, LANES), jnp.bfloat16),
            pltpu.VMEM((BINS // LANES, 8, LANES), jnp.float32),
            pltpu.VMEM((2, split * state + EXTRA, width), jnp.float32),
            sums(chips), sums(chips), stats(chips), stats(chips),
            sums(chips), sums(chips + 1), stats(chips), stats(chips + 1),
            pltpu.VMEM((chips, 4, LANES), jnp.float32),
            pltpu.VMEM((8, LANES), jnp.float32),
            pltpu.VMEM((8, LANES), jnp.float32),
            pltpu.VMEM((groups - 1, 8, LANES), jnp.float32),
            pltpu.SemaphoreType.DMA,
            pltpu.SemaphoreType.DMA((2, chips)),
            pltpu.SemaphoreType.DMA((2, chips)),
            pltpu.SemaphoreType.DMA((2, chips)),
            pltpu.SemaphoreType.DMA((2, chips + 1)),
            pltpu.SemaphoreType.DMA((groups - 1,)),
            pltpu.SemaphoreType.DMA((groups - 1,)),
        ],
        compiler_params=pltpu.CompilerParams(
            collective_id=0, has_side_effects=True, vmem_limit_bytes=52 * 1024 * 1024),
    )(log_weights.reshape(rows, LANES), bins.reshape(rows, LANES), states)
    cumulative, bin_means, weights = pl.pallas_call(
        drain,
        out_shape=shapes,
        in_specs=[vmem, vmem, vmem],
        out_specs=(hbm, hbm, hbm),
        scratch_shapes=[pltpu.SemaphoreType.DMA((3,))],
        compiler_params=pltpu.CompilerParams(vmem_limit_bytes=4 * 1024 * 1024),
    )(*found)
    return cumulative.reshape(owned), bin_means, weights.reshape(count)


def solution(mesh):
    placed = (P(("filt", "dom")), P(("filt", "dom")), P(None, ("filt", "dom")))
    return jax.shard_map(
        body,
        mesh=mesh,
        in_specs=placed,
        out_specs=(P(("filt", "dom")), P(None, ("filt", "dom")), P(("filt", "dom"))),
        check_vma=False,
    )
```

```python
import functools

import jax
import jax.numpy as jnp
from jax import lax
from jax.experimental import pallas as pl
from jax.experimental.pallas import tpu as pltpu
from jax.sharding import PartitionSpec as P

BINS = 4096
LANES = 128
LEVEL_BITS = 20
LEVELS = 1 << LEVEL_BITS
LEAST = -20.0
PER_UNIT = (LEVELS - 3) / 270.0

floor_value = -10000.0


def spread_rows(ref, values):
    for r in range(values.shape[0]):
        ref[16 * r:16 * r + 16, :] = jnp.broadcast_to(values[r:r + 1, :], (16, LANES)).astype(ref.dtype)


def sort_keys(keys):
    tile_bits = len(keys).bit_length() - 1
    bits = tile_bits + 10
    sub = lax.broadcasted_iota(jnp.int32, (8, LANES), 0)
    lane = lax.broadcasted_iota(jnp.int32, (8, LANES), 1)

    def mask_of(bit):
        if bit < tile_bits + 3:
            return (sub >> (bit - tile_bits)) & 1
        return (lane >> (bit - tile_bits - 3)) & 1

    def turned(size):
        if size >= bits:
            return None
        if size < tile_bits:
            return [-((t >> size) & 1) for t in range(len(keys))]
        return -mask_of(size)

    def flip(now, then):
        for t in range(len(keys)):
            a = now[t] if isinstance(now, list) else now
            b = then[t] if isinstance(then, list) else then
            if a is None:
                a = 0
            if b is None:
                b = 0
            if isinstance(a, int) and isinstance(b, int):
                if a != b:
                    keys[t] = ~keys[t]
                continue
            keys[t] = keys[t] ^ (a ^ b)

    before = None
    for size in range(1, bits + 1):
        down = turned(size)
        flip(before, down)
        before = down
        for bit in range(size - 1, -1, -1):
            if bit < tile_bits:
                for t in range(len(keys)):
                    o = t | (1 << bit)
                    if o != t:
                        keys[t], keys[o] = jnp.minimum(keys[t], keys[o]), jnp.maximum(keys[t], keys[o])
                continue
            upper = mask_of(bit) != 0
            if bit < tile_bits + 3:
                index, axis = sub ^ (1 << (bit - tile_bits)), 0
            else:
                index, axis = lane ^ (1 << (bit - tile_bits - 3)), 1
            for t in range(len(keys)):
                k = jnp.take_along_axis(keys[t], index, axis=axis)
                keys[t] = jnp.where(upper, jnp.maximum(keys[t], k), jnp.minimum(keys[t], k))
    return keys


def local_tops(lw, bins):
    count = lw.shape[0] // 8
    table = BINS // LANES
    level = jnp.clip((lw - LEAST) * PER_UNIT + 1.5, 1.0, float(LEVELS - 1)).astype(jnp.int32)
    packed = (bins - BINS // 2) * LEVELS + level
    keys = sort_keys([packed[8 * t:8 * t + 8] for t in range(count)])
    sub = lax.broadcasted_iota(jnp.int32, (8, LANES), 0)
    lane = lax.broadcasted_iota(jnp.int32, (8, LANES), 1)
    places = [(k >> LEVEL_BITS) + BINS // 2 for k in keys]
    turned = pltpu.roll(places[0], 7, 0)
    following = jnp.where(sub == 7, pltpu.roll(turned, LANES - 1, 1), turned)
    following = jnp.where((sub == 7) & (lane == LANES - 1), -1, following)
    high_label = lax.broadcasted_iota(jnp.int32, (table, LANES), 0).astype(jnp.float32).astype(jnp.bfloat16)
    low_label = lax.broadcasted_iota(jnp.int32, (LANES, LANES), 0).astype(jnp.float32).astype(jnp.bfloat16)
    zero, one = jnp.zeros((), jnp.bfloat16), jnp.ones((), jnp.bfloat16)
    found = jnp.zeros((3 * table, LANES), jnp.float32)

    def row(x, r):
        return jnp.broadcast_to(x[r:r + 1], (16, LANES)).astype(jnp.bfloat16)

    for t in range(count):
        last = places[t] != (places[t + 1] if t + 1 < count else following)
        high = jnp.where(last, places[t] // LANES, -1).astype(jnp.float32)
        low = (places[t] % LANES).astype(jnp.float32)
        size = keys[t] & (LEVELS - 1)
        parts = [(size >> 12).astype(jnp.float32), ((size >> 4) & 255).astype(jnp.float32),
                 (size & 15).astype(jnp.float32)]
        left, right = [], []
        for r in range(8):
            member = jnp.concatenate([row(high, r)] * (table // 16), axis=0) == high_label
            left.append(jnp.concatenate(
                [jnp.where(member, jnp.concatenate([row(x, r)] * (table // 16), axis=0), zero) for x in parts], axis=0))
            right.append(jnp.where(jnp.concatenate([row(low, r)] * (LANES // 16), axis=0) == low_label, one, zero))
        found = found + lax.dot_general(jnp.concatenate(left, axis=1), jnp.concatenate(right, axis=1),
                                        (((1,), (1,)), ((), ())), preferred_element_type=jnp.float32)
    top = (found[0:table] * 4096.0 + found[table:2 * table] * 16.0) + found[2 * table:3 * table]
    return jnp.where(top > 0.5, (top - 1.0) * (1.0 / PER_UNIT) + LEAST, floor_value)


def plan(chips):
    if chips == 4:
        order = [[3, 1, 2, 0], [2, 3, 0, 1], [1, 0, 3, 2], [0, 2, 1, 3]]
        target = [[1, 1, 2], [2, 3, 0], [1, 0, 3], [2, 2, 1]]
        merged = [[1, 0, 0], [0, 0, 0], [0, 0, 0], [1, 0, 0]]
        return order, target, merged, {1: (1, 2)}, {(0, 3), (3, 0)}
    order = [sorted((d for d in range(chips) if d != c), key=lambda d: -abs(d - c)) + [c] for c in range(chips)]
    target = [o[:-1] for o in order]
    merged = [[0] * (chips - 1) for _ in range(chips)]
    return order, target, merged, {}, set()


def pick(table, chip):
    value = table[0]
    for c in range(1, len(table)):
        if table[c] != table[c - 1]:
            value = value + jnp.where(chip >= c, table[c] - table[c - 1], 0)
    return value


def kernel(groups, whole_count, lw_ref, bins_ref, states_hbm, cum_ref, means_ref, weights_ref,
           held, ext, lo_b, hi_b, part_b, w_b, top_tab, mass_tab, blocks,
           tops_send, tops_recv, mass_send, mass_recv, pair_send, pair_recv, by_mine, by_theirs,
           send, recv, send_s, recv_s, fac, stat_send, stat_recv,
           load_sem, table_ss, table_rs, pair_ss, pair_rs, chip_ss, chip_rs, word_ss, word_rs, stat_ss, stat_rs):
    state = held.shape[0]
    count = held.shape[1]
    rows = count // LANES
    owned = BINS // groups
    both = 2 * owned
    width = min(256, owned)
    half = owned // width
    chunks = owned // LANES
    per = width // LANES
    chips = groups // 2
    units = chips * half
    last = chips - 1
    order, target, merged, merging, skipped = plan(chips)
    me = lax.axis_index("dom")
    chip, core = me // 2, me % 2
    dests = [pick([o[s] for o in order], chip) for s in range(chips)]

    load = pltpu.make_async_copy(states_hbm, held, load_sem)
    load.start()
    barrier = pltpu.get_barrier_semaphore()
    for k in range(1, groups):
        pl.semaphore_signal(barrier, inc=1, device_id={"dom": lax.rem(me + k, groups)},
                            device_id_type=pl.DeviceIdType.MESH)

    lw = lw_ref[...]
    bins = bins_ref[...]
    spread_rows(lo_b, (bins % width).astype(jnp.float32))
    spread_rows(hi_b, (bins // both).astype(jnp.float32))
    spread_rows(part_b, ((bins % both) // width).astype(jnp.float32))
    tops = local_tops(lw, bins)
    low, high = bins % LANES, bins // LANES
    own_top = jnp.zeros(lw.shape, jnp.float32)
    for t in range(BINS // LANES):
        picked = jnp.take_along_axis(jnp.broadcast_to(tops[t:t + 1], lw.shape), low, axis=1)
        own_top = jnp.where(high == t, picked, own_top)
        top_tab[t] = jnp.broadcast_to(tops[t:t + 1], (8, LANES))
    spread_rows(w_b, jnp.exp(lw - own_top))
    load.wait()

    zero = jnp.zeros((), jnp.bfloat16)

    def mask_states(p):
        def step(r, carry):
            part = part_b[pl.ds(pl.multiple_of(r * 16, 16), 16), :]
            cols = pl.ds(pl.multiple_of(r * LANES, LANES), LANES)
            tile = held[:, cols]
            part_all = jnp.concatenate([part] * (state // 16), axis=0)
            for k in range(2):
                at = (2 * p + k) * state
                ext[at:at + state, cols] = jnp.where(part_all == jnp.bfloat16(k * half + p), tile, zero)
            return carry

        lax.fori_loop(0, rows, step, 0)

    label = lax.broadcasted_iota(jnp.int32, (width, LANES), 0).astype(jnp.float32).astype(jnp.bfloat16)

    def product(dest, p, c, depth):
        tile = jnp.asarray(dest).astype(jnp.float32).astype(jnp.bfloat16)
        pieces = []
        for j in range(depth):
            at = pl.ds(pl.multiple_of((c * depth + j) * 16, 16), 16)
            w = jnp.where(hi_b[at, :] == tile, w_b[at, :], zero)
            lo = lo_b[at, :]
            w_all = jnp.concatenate([w] * (width // 16), axis=0)
            lo_all = jnp.concatenate([lo] * (width // 16), axis=0)
            pieces.append(jnp.where(lo_all == label, w_all, zero))
        spread = jnp.concatenate(pieces, axis=1)
        cols = pl.ds(pl.multiple_of(c * depth * LANES, LANES), depth * LANES)
        left = ext[pl.ds(pl.multiple_of(2 * p * state, 2 * state), 2 * state), cols]
        return lax.dot_general(left, spread, (((1,), (1,)), ((), ())), preferred_element_type=jnp.float32)

    def mass_table():
        side = 64
        depth = min(32, rows)
        per_row = BINS // side
        low_label = lax.broadcasted_iota(jnp.int32, (side, LANES), 0).astype(jnp.float32).astype(jnp.bfloat16)
        turn = lax.broadcasted_iota(jnp.int32, (per_row, LANES), 0)
        turn = 2 * (turn % (per_row // 2)) + turn // (per_row // 2)
        high_label = turn.astype(jnp.float32).astype(jnp.bfloat16)
        one = jnp.ones((), jnp.bfloat16)

        def step(c, carry):
            left, right = [], []
            for j in range(depth):
                at = pl.ds(pl.multiple_of((c * depth + j) * 16, 16), 16)
                lo = lo_b[at, :]
                high = hi_b[at, :] * jnp.bfloat16(both // side) + part_b[at, :] * jnp.bfloat16(width // side)
                step = width // 2
                while step >= side:
                    over = lo >= jnp.bfloat16(step)
                    lo = jnp.where(over, lo - jnp.bfloat16(step), lo)
                    high = jnp.where(over, high + jnp.bfloat16(step // side), high)
                    step //= 2
                w = w_b[at, :]
                left.append(jnp.where(jnp.concatenate([high] * (per_row // 16), axis=0) == high_label,
                                      jnp.concatenate([w] * (per_row // 16), axis=0), zero))
                right.append(jnp.where(jnp.concatenate([lo] * (side // 16), axis=0) == low_label, one, zero))
            return carry + lax.dot_general(jnp.concatenate(left, axis=1), jnp.concatenate(right, axis=1),
                                           (((1,), (1,)), ((), ())), preferred_element_type=jnp.float32)

        found = lax.fori_loop(0, rows // depth, step, jnp.zeros((per_row, side), jnp.float32))
        found = jnp.concatenate([found[0:per_row // 2], found[per_row // 2:]], axis=1)
        for t in range(BINS // LANES):
            mass_tab[t] = jnp.broadcast_to(found[t:t + 1], (8, LANES))

    def remote(src, dst, ss, rs, chip_to, core_to):
        return pltpu.make_async_remote_copy(src, dst, ss, rs, device_id={"dom": chip_to * 2 + core_to},
                                            device_id_type=pl.DeviceIdType.MESH)

    def rows_of(table, dest, which):
        found = [table[(dest * 2 + which) * chunks + j][0:1] for j in range(chunks)]
        pad = [jnp.zeros((4 - chunks, LANES), jnp.float32)] if chunks < 4 else []
        return jnp.concatenate(found + pad, axis=0)

    def table_copy(which):
        src, dst = ((tops_send, tops_recv), (mass_send, mass_recv))[which]
        return remote(src, dst, table_ss.at[which], table_rs.at[which], chip, 1 - core)

    def pair_copy(u):
        return remote(pair_send.at[u], pair_recv.at[u], pair_ss.at[u], pair_rs.at[u], chip, 1 - core)

    def piece(p):
        return pl.ds(pl.multiple_of(p * per * state, per * state), per * state)

    def chunk(j):
        return pl.ds(pl.multiple_of(j * state, state), state)

    def incoming(slot, p):
        return remote(send.at[0, piece(p)], recv.at[slot, piece(p)], chip_ss.at[0], chip_rs.at[slot, p], chip, 1 - core)

    def incoming_word(slot):
        return remote(send_s.at[0], recv_s.at[slot], word_ss.at[0], word_rs.at[slot], chip, 1 - core)

    def at_step(values, s):
        found = values[0]
        for k in range(1, len(values)):
            found = found + jnp.where(s == k, values[k] - values[0], 0)
        return found

    targets = [pick([t[s] for t in target], chip) for s in range(last)]
    slots = [chip + pick([m[s] for m in merged], chip) * (chips - chip) for s in range(last)]

    def outgoing(u):
        s, p = u // half, u % half
        return remote(send.at[s, piece(p)], recv.at[at_step(slots, s), piece(p)], chip_ss.at[u],
                      chip_rs.at[at_step(slots, s), p], at_step(targets, s), core)

    def outgoing_word(s):
        return remote(send_s.at[s], recv_s.at[slots[s]], word_ss.at[s], word_rs.at[slots[s]], targets[s], core)

    def merges(s):
        first, final = merging[s]
        return (chip >= first) & (chip <= final)

    def give(u):
        found = blocks[u % 2, pl.ds(pl.multiple_of((1 - core) * state, state), state)]
        for l in range(per):
            pair_send[u, l * state:(l + 1) * state] = found[:, l * LANES:(l + 1) * LANES]
        pair_copy(u).start()

    def keep(table, s, values):
        for j in range(chunks):
            table[s * chunks + j] = jnp.broadcast_to(values[j:j + 1], (8, LANES))

    def handle_tops():
        table_copy(0).wait_recv()
        for s in range(chips):
            mine, theirs = rows_of(top_tab, dests[s], core), tops_recv[s]
            most = jnp.maximum(mine, theirs)
            keep(by_mine, s, jnp.exp(mine - most))
            keep(by_theirs, s, jnp.exp(theirs - most))
            send_s[s, 4:8] = most

    def handle_masses():
        table_copy(1).wait_recv()
        for s in range(chips):
            for j in range(chunks):
                mine = mass_tab[(dests[s] * 2 + core) * chunks + j][0:1]
                send_s[s, j:j + 1] = (mine * by_mine[s * chunks + j, 0:1]
                                      + mass_recv[s, j:j + 1] * by_theirs[s * chunks + j, 0:1])
            for j in range(chunks, 4):
                send_s[s, j:j + 1] = jnp.zeros((1, LANES), jnp.float32)
            if s < last and s not in merging:
                outgoing_word(s).start()

    def scale_step(s, values):
        for j in range(chunks):
            by_mine[s * chunks + j] = by_mine[s * chunks + j] * values[j:j + 1]
            by_theirs[s * chunks + j] = by_theirs[s * chunks + j] * values[j:j + 1]

    def merge_words(s):
        @pl.when(merges(s))
        def _():
            incoming_word(chips).wait_recv()
            mine, theirs = send_s[s, 4:8], recv_s[chips, 4:8]
            most = jnp.maximum(mine, theirs)
            to_mine, to_theirs = jnp.exp(mine - most), jnp.exp(theirs - most)
            scale_step(s, to_mine)
            keep(fac, chips, to_theirs)
            send_s[s, 0:4] = send_s[s, 0:4] * to_mine + recv_s[chips, 0:4] * to_theirs
            send_s[s, 4:8] = most

        outgoing_word(s).start()

    def handle(u):
        s, p = u // half, u % half
        for m in merging:
            @pl.when(u == m * half)
            def _(m=m):
                merge_words(m)
        pair_copy(u).wait_recv()
        found = blocks[u % 2, pl.ds(pl.multiple_of(core * state, state), state)]
        for l in range(per):
            j = p * per + l
            send[s, chunk(j)] = (
                found[:, l * LANES:(l + 1) * LANES] * by_mine[s * chunks + j, 0:1]
                + pair_recv[u, l * state:(l + 1) * state] * by_theirs[s * chunks + j, 0:1])
        for m in merging:
            @pl.when((s == m) & merges(m))
            def _(m=m):
                incoming(chips, p).wait_recv()
                for l in range(per):
                    j = p * per + l
                    send[m, chunk(j)] = send[m, chunk(j)] + recv[chips, chunk(j)] * fac[chips * chunks + j, 0:1]

        @pl.when(s < last)
        def _():
            outgoing(u).start()

    def valid(sender):
        ok = chip != sender
        for owner, other in skipped:
            if other == sender:
                ok = ok & (chip != owner)
        return ok

    real = lax.broadcasted_iota(jnp.int32, (4, LANES), 0) < chunks

    def stat_copies():
        return [pltpu.make_async_remote_copy(
            stat_send, stat_recv.at[k - 1], stat_ss.at[k - 1], stat_rs.at[k - 1],
            device_id={"dom": lax.rem(me + k, groups)}, device_id_type=pl.DeviceIdType.MESH)
            for k in range(1, groups)]

    def owned_words():
        for c in range(chips):
            @pl.when(valid(c))
            def _(c=c):
                incoming_word(c).wait_recv()

            @pl.when(jnp.logical_not(valid(c)))
            def _(c=c):
                recv_s[c, 0:4] = jnp.zeros((4, LANES), jnp.float32)
                recv_s[c, 4:8] = jnp.full((4, LANES), floor_value, jnp.float32)

        own = send_s[last, 4:8]
        bin_top = own
        for c in range(chips):
            bin_top = jnp.maximum(bin_top, recv_s[c, 4:8])
        by_own = jnp.exp(own - bin_top)
        mass = send_s[last, 0:4] * by_own
        for c in range(chips):
            by = jnp.exp(recv_s[c, 4:8] - bin_top)
            keep(fac, c, by)
            mass = mass + recv_s[c, 0:4] * by
        scale_step(last, by_own)
        block_top = jnp.max(jnp.max(jnp.where(real, bin_top, floor_value), axis=1, keepdims=True), axis=0,
                            keepdims=True)
        share = jnp.where(real, mass * jnp.exp(bin_top - block_top), 0.0)
        block_mass = jnp.sum(jnp.sum(share, axis=1, keepdims=True), axis=0, keepdims=True)
        send_s[last, 0:4] = mass
        send_s[last, 4:8] = share
        stat_send[0:4, :] = jnp.broadcast_to(block_top, (4, LANES))
        stat_send[4:8, :] = jnp.broadcast_to(block_mass, (4, LANES))
        for copy in stat_copies():
            copy.start()

    def close_stats():
        share = send_s[last, 4:8]
        run = share
        position = lax.broadcasted_iota(jnp.int32, run.shape, 1)
        hop = 1
        while hop < LANES:
            run = run + jnp.where(position >= hop, pltpu.roll(run, hop, 1), 0.0)
            hop *= 2
        base = jnp.zeros((1, 1), jnp.float32)
        runs = []
        for j in range(chunks):
            runs.append(run[j:j + 1] + base)
            base = base + run[j:j + 1, LANES - 1:LANES]
        for copy in stat_copies():
            copy.wait_recv()
        block_top, block_mass = stat_send[0:1, 0:1], stat_send[4:5, 0:1]
        top = block_top
        for k in range(groups - 1):
            top = jnp.maximum(top, stat_recv[k, 0:1, 0:1])
        scale = jnp.exp(block_top - top)
        total = block_mass * scale
        before = jnp.zeros_like(total)
        for k in range(groups - 1):
            theirs = stat_recv[k, 4:5, 0:1] * jnp.exp(stat_recv[k, 0:1, 0:1] - top)
            total = total + theirs
            before = before + jnp.where(me >= k + 1, theirs, 0.0)
        cum_ref[...] = (before + jnp.concatenate(runs, axis=1) * scale) / total
        weights_ref[...] = whole_count * jnp.exp(lw_ref[...] - top) / total

    for s in range(chips):
        tops_send[s] = rows_of(top_tab, dests[s], 1 - core)
    mask_states(0)
    pl.semaphore_wait(barrier, groups - 1)
    table_copy(0).start()
    depth = min(64, rows) if chips <= 4 else min(16, rows)
    steps = rows // depth

    def turn(v, carry):
        u, c = v // steps, v % steps
        s, p = u // half, u % half
        found = blocks.at[u % 2]
        added = product(at_step(dests, s), p, c, depth)

        found[...] = jnp.where(c > 0, found[...], 0.0) + added

        @pl.when(v == 2 * steps - 1)
        def _():
            handle_masses()

        @pl.when(v == (units - 1) * steps)
        def _():
            owned_words()

        @pl.when((c == 0) & (u > 1))
        def _():
            handle(u - 1)

        @pl.when(c == steps - 1)
        def _():
            give(u)

        @pl.when(v == steps - 1)
        def _():
            for q in range(1, half):
                mask_states(q)
            mass_table()
            for t in range(chips):
                mass_send[t] = rows_of(mass_tab, dests[t], 1 - core)
            table_copy(1).start()
            handle_tops()
            handle(0)

        return carry

    lax.fori_loop(0, units * steps, turn, 0)
    handle(units - 1)
    close_stats()
    for c in range(chips):
        @pl.when(valid(c))
        def _(c=c):
            for p in range(half):
                incoming(c, p).wait_recv()
            for j in range(chunks):
                at = slice(j * state, (j + 1) * state)
                send[last, at] = send[last, at] + recv[c, at] * fac[c * chunks + j, 0:1]
    for j in range(chunks):
        means_ref[:, j * LANES:(j + 1) * LANES] = (send[last, j * state:(j + 1) * state]
                                                   / jnp.maximum(send_s[last, j:j + 1], 1.0))
    for which in range(2):
        table_copy(which).wait_send()
    for u in range(units):
        pair_copy(u).wait_send()
    for u in range(last * half):
        outgoing(u).wait_send()
    for s in range(last):
        outgoing_word(s).wait_send()
    for copy in stat_copies():
        copy.wait_send()


def drain(*refs):
    sources, results, sems = refs[0:3], refs[3:6], refs[6]
    copies = [pltpu.make_async_copy(sources[i], results[i], sems.at[i]) for i in range(3)]
    for copy in copies:
        copy.start()
    for copy in copies:
        copy.wait()


def body(log_weights, bins, states):
    groups = lax.axis_size("dom")
    owned = BINS // groups
    chips = groups // 2
    state, count = states.shape
    rows = count // LANES
    width = min(256, owned)
    chunks = owned // LANES
    vmem = pl.BlockSpec(memory_space=pltpu.VMEM)
    hbm = pl.BlockSpec(memory_space=pltpu.HBM)

    half = owned // width
    units = chips * half

    def sums(slots):
        return pltpu.VMEM((slots, chunks * state, LANES), jnp.float32)

    def words(slots, depth=8):
        return pltpu.VMEM((slots, depth, LANES), jnp.float32)

    def spread():
        return pltpu.VMEM((rows * 16, LANES), jnp.bfloat16)

    shapes = (jax.ShapeDtypeStruct((1, owned), jnp.float32),
              jax.ShapeDtypeStruct((state, owned), jnp.float32),
              jax.ShapeDtypeStruct((rows, LANES), jnp.float32))
    found = pl.pallas_call(
        functools.partial(kernel, groups, float(count * groups)),
        out_shape=shapes,
        in_specs=[vmem, vmem, hbm],
        out_specs=(vmem, vmem, vmem),
        scratch_shapes=[
            pltpu.VMEM((state, count), jnp.bfloat16),
            pltpu.VMEM((2 * half * state, count), jnp.bfloat16),
            spread(), spread(), spread(), spread(),
            words(BINS // LANES), words(BINS // LANES),
            pltpu.VMEM((2, 2 * state, width), jnp.float32),
            words(chips, 4), words(chips, 4), words(chips, 4), words(chips, 4),
            pltpu.VMEM((units, (width // LANES) * state, LANES), jnp.float32),
            pltpu.VMEM((units, (width // LANES) * state, LANES), jnp.float32),
            words(chips * chunks), words(chips * chunks),
            sums(chips), sums(chips + 1), words(chips), words(chips + 1), words((chips + 1) * chunks),
            pltpu.VMEM((8, LANES), jnp.float32),
            words(groups - 1),
            pltpu.SemaphoreType.DMA,
            pltpu.SemaphoreType.DMA((2,)),
            pltpu.SemaphoreType.DMA((2,)),
            pltpu.SemaphoreType.DMA((units,)),
            pltpu.SemaphoreType.DMA((units,)),
            pltpu.SemaphoreType.DMA((units,)),
            pltpu.SemaphoreType.DMA((chips + 1, half)),
            pltpu.SemaphoreType.DMA((chips,)),
            pltpu.SemaphoreType.DMA((chips + 1,)),
            pltpu.SemaphoreType.DMA((groups - 1,)),
            pltpu.SemaphoreType.DMA((groups - 1,)),
        ],
        compiler_params=pltpu.CompilerParams(
            collective_id=0, has_side_effects=True, vmem_limit_bytes=52 * 1024 * 1024),
    )(log_weights.reshape(rows, LANES), bins.reshape(rows, LANES), states)
    cumulative, bin_means, weights = pl.pallas_call(
        drain,
        out_shape=shapes,
        in_specs=[vmem, vmem, vmem],
        out_specs=(hbm, hbm, hbm),
        scratch_shapes=[pltpu.SemaphoreType.DMA((3,))],
        compiler_params=pltpu.CompilerParams(vmem_limit_bytes=4 * 1024 * 1024),
    )(*found)
    return cumulative.reshape(owned), bin_means, weights.reshape(count)


def solution(mesh):
    placed = (P(("filt", "dom")), P(("filt", "dom")), P(None, ("filt", "dom")))
    return jax.shard_map(
        body,
        mesh=mesh,
        in_specs=placed,
        out_specs=(P(("filt", "dom")), P(None, ("filt", "dom")), P(("filt", "dom"))),
        check_vma=False,
    )
```

```python
import functools

import jax
import jax.numpy as jnp
from jax import lax
from jax.experimental import pallas as pl
from jax.experimental.pallas import tpu as pltpu
from jax.sharding import PartitionSpec as P

BINS = 4096
LANES = 128
LEVEL_BITS = 20
LEVELS = 1 << LEVEL_BITS
LEAST = -20.0
PER_UNIT = (LEVELS - 3) / 270.0

floor_value = -10000.0


def spread_rows(ref, values):
    for r in range(values.shape[0]):
        ref[16 * r:16 * r + 16, :] = jnp.broadcast_to(values[r:r + 1, :], (16, LANES)).astype(ref.dtype)


def sort_keys(keys):
    tile_bits = len(keys).bit_length() - 1
    bits = tile_bits + 10
    sub = lax.broadcasted_iota(jnp.int32, (8, LANES), 0)
    lane = lax.broadcasted_iota(jnp.int32, (8, LANES), 1)

    def mask_of(bit):
        if bit < tile_bits + 3:
            return (sub >> (bit - tile_bits)) & 1
        return (lane >> (bit - tile_bits - 3)) & 1

    def turned(size):
        if size >= bits:
            return None
        if size < tile_bits:
            return [-((t >> size) & 1) for t in range(len(keys))]
        return -mask_of(size)

    def flip(now, then):
        for t in range(len(keys)):
            a = now[t] if isinstance(now, list) else now
            b = then[t] if isinstance(then, list) else then
            if a is None:
                a = 0
            if b is None:
                b = 0
            if isinstance(a, int) and isinstance(b, int):
                if a != b:
                    keys[t] = ~keys[t]
                continue
            keys[t] = keys[t] ^ (a ^ b)

    before = None
    for size in range(1, bits + 1):
        down = turned(size)
        flip(before, down)
        before = down
        for bit in range(size - 1, -1, -1):
            if bit < tile_bits:
                for t in range(len(keys)):
                    o = t | (1 << bit)
                    if o != t:
                        keys[t], keys[o] = jnp.minimum(keys[t], keys[o]), jnp.maximum(keys[t], keys[o])
                continue
            upper = mask_of(bit) != 0
            if bit < tile_bits + 3:
                index, axis = sub ^ (1 << (bit - tile_bits)), 0
            else:
                index, axis = lane ^ (1 << (bit - tile_bits - 3)), 1
            for t in range(len(keys)):
                k = jnp.take_along_axis(keys[t], index, axis=axis)
                keys[t] = jnp.where(upper, jnp.maximum(keys[t], k), jnp.minimum(keys[t], k))
    return keys


def local_tops(lw, bins):
    count = lw.shape[0] // 8
    table = BINS // LANES
    level = jnp.clip((lw - LEAST) * PER_UNIT + 1.5, 1.0, float(LEVELS - 1)).astype(jnp.int32)
    packed = (bins - BINS // 2) * LEVELS + level
    keys = sort_keys([packed[8 * t:8 * t + 8] for t in range(count)])
    sub = lax.broadcasted_iota(jnp.int32, (8, LANES), 0)
    lane = lax.broadcasted_iota(jnp.int32, (8, LANES), 1)
    places = [(k >> LEVEL_BITS) + BINS // 2 for k in keys]
    turned = pltpu.roll(places[0], 7, 0)
    following = jnp.where(sub == 7, pltpu.roll(turned, LANES - 1, 1), turned)
    following = jnp.where((sub == 7) & (lane == LANES - 1), -1, following)
    high_label = lax.broadcasted_iota(jnp.int32, (table, LANES), 0).astype(jnp.float32).astype(jnp.bfloat16)
    low_label = lax.broadcasted_iota(jnp.int32, (LANES, LANES), 0).astype(jnp.float32).astype(jnp.bfloat16)
    zero, one = jnp.zeros((), jnp.bfloat16), jnp.ones((), jnp.bfloat16)
    found = jnp.zeros((3 * table, LANES), jnp.float32)

    def row(x, r):
        return jnp.broadcast_to(x[r:r + 1], (16, LANES)).astype(jnp.bfloat16)

    for t in range(count):
        last = places[t] != (places[t + 1] if t + 1 < count else following)
        high = jnp.where(last, places[t] // LANES, -1).astype(jnp.float32)
        low = (places[t] % LANES).astype(jnp.float32)
        size = keys[t] & (LEVELS - 1)
        parts = [(size >> 12).astype(jnp.float32), ((size >> 4) & 255).astype(jnp.float32),
                 (size & 15).astype(jnp.float32)]
        left, right = [], []
        for r in range(8):
            member = jnp.concatenate([row(high, r)] * (table // 16), axis=0) == high_label
            left.append(jnp.concatenate(
                [jnp.where(member, jnp.concatenate([row(x, r)] * (table // 16), axis=0), zero) for x in parts], axis=0))
            right.append(jnp.where(jnp.concatenate([row(low, r)] * (LANES // 16), axis=0) == low_label, one, zero))
        found = found + lax.dot_general(jnp.concatenate(left, axis=1), jnp.concatenate(right, axis=1),
                                        (((1,), (1,)), ((), ())), preferred_element_type=jnp.float32)
    top = (found[0:table] * 4096.0 + found[table:2 * table] * 16.0) + found[2 * table:3 * table]
    return jnp.where(top > 0.5, (top - 1.0) * (1.0 / PER_UNIT) + LEAST, floor_value)


def plan(chips):
    if chips == 4:
        order = [[3, 1, 2, 0], [2, 3, 0, 1], [1, 0, 3, 2], [0, 2, 1, 3]]
        target = [[1, 1, 2], [2, 3, 0], [1, 0, 3], [2, 2, 1]]
        merged = [[1, 0, 0], [0, 0, 0], [0, 0, 0], [1, 0, 0]]
        return order, target, merged, {1: (1, 2)}, {(0, 3), (3, 0)}
    order = [sorted((d for d in range(chips) if d != c), key=lambda d: -abs(d - c)) + [c] for c in range(chips)]
    target = [o[:-1] for o in order]
    merged = [[0] * (chips - 1) for _ in range(chips)]
    return order, target, merged, {}, set()


def pick(table, chip):
    value = table[0]
    for c in range(1, len(table)):
        if table[c] != table[c - 1]:
            value = value + jnp.where(chip >= c, table[c] - table[c - 1], 0)
    return value


def kernel(groups, whole_count, lw_ref, bins_ref, states_hbm, cum_ref, means_ref, weights_ref,
           held, ext, lo_b, hi_b, part_b, w_b, top_tab, mass_tab, blocks,
           tops_send, tops_recv, mass_send, mass_recv, pair_send, pair_recv, by_mine, by_theirs,
           send, recv, send_s, recv_s, fac, stat_send, stat_recv,
           load_sem, table_ss, table_rs, pair_ss, pair_rs, chip_ss, chip_rs, word_ss, word_rs, stat_ss, stat_rs):
    state = held.shape[0]
    count = held.shape[1]
    rows = count // LANES
    owned = BINS // groups
    both = 2 * owned
    width = min(256, owned)
    half = owned // width
    chunks = owned // LANES
    per = width // LANES
    chips = groups // 2
    units = chips * half
    last = chips - 1
    order, target, merged, merging, skipped = plan(chips)
    me = lax.axis_index("dom")
    chip, core = me // 2, me % 2
    dests = [pick([o[s] for o in order], chip) for s in range(chips)]

    load = pltpu.make_async_copy(states_hbm, held, load_sem)
    load.start()
    barrier = pltpu.get_barrier_semaphore()
    for k in range(1, groups):
        pl.semaphore_signal(barrier, inc=1, device_id={"dom": lax.rem(me + k, groups)},
                            device_id_type=pl.DeviceIdType.MESH)

    lw = lw_ref[...]
    bins = bins_ref[...]
    spread_rows(lo_b, (bins % width).astype(jnp.float32))
    spread_rows(hi_b, (bins // both).astype(jnp.float32))
    spread_rows(part_b, ((bins % both) // width).astype(jnp.float32))
    tops = local_tops(lw, bins)
    low, high = bins % LANES, bins // LANES
    own_tops = []
    for v in range(rows // 8):
        at = slice(8 * v, 8 * v + 8)
        found = jnp.zeros((8, LANES), jnp.float32)
        for t in range(BINS // LANES):
            picked = jnp.take_along_axis(jnp.broadcast_to(tops[t:t + 1], (8, LANES)), low[at], axis=1)
            found = jnp.where(high[at] == t, picked, found)
        own_tops.append(found)
    own_top = jnp.concatenate(own_tops, axis=0)
    for t in range(BINS // LANES):
        top_tab[t] = jnp.broadcast_to(tops[t:t + 1], (8, LANES))
    spread_rows(w_b, jnp.exp(lw - own_top))
    load.wait()

    zero = jnp.zeros((), jnp.bfloat16)

    def mask_states(p):
        def step(r, carry):
            for i in range(4):
                part = part_b[pl.ds(pl.multiple_of((4 * r + i) * 16, 16), 16), :]
                tile = held[:, pl.ds(pl.multiple_of((4 * r + i) * LANES, LANES), LANES)]
                part_all = jnp.concatenate([part] * (state // 16), axis=0)
                for k in range(2):
                    at = (2 * p + k) * state
                    ext[4 * r + i, at:at + state] = jnp.where(part_all == jnp.bfloat16(k * half + p), tile, zero)
            return carry

        lax.fori_loop(0, rows // 4, step, 0)

    label = lax.broadcasted_iota(jnp.int32, (width, LANES), 0).astype(jnp.float32).astype(jnp.bfloat16)

    def product(dest, p, c, depth):
        tile = jnp.asarray(dest).astype(jnp.float32).astype(jnp.bfloat16)
        pieces = []
        for j in range(depth):
            at = pl.ds(pl.multiple_of((c * depth + j) * 16, 16), 16)
            w = jnp.where(hi_b[at, :] == tile, w_b[at, :], zero)
            lo = lo_b[at, :]
            w_all = jnp.concatenate([w] * (width // 16), axis=0)
            lo_all = jnp.concatenate([lo] * (width // 16), axis=0)
            pieces.append(jnp.where(lo_all == label, w_all, zero))
        spread = jnp.concatenate(pieces, axis=1)
        at = pl.ds(pl.multiple_of(2 * p * state, 2 * state), 2 * state)
        left = jnp.concatenate([ext[c * depth + j, at] for j in range(depth)], axis=1)
        return lax.dot_general(left, spread, (((1,), (1,)), ((), ())), preferred_element_type=jnp.float32)

    def mass_table():
        side = 64
        depth = min(32, rows)
        per_row = BINS // side
        low_label = lax.broadcasted_iota(jnp.int32, (side, LANES), 0).astype(jnp.float32).astype(jnp.bfloat16)
        turn = lax.broadcasted_iota(jnp.int32, (per_row, LANES), 0)
        turn = 2 * (turn % (per_row // 2)) + turn // (per_row // 2)
        high_label = turn.astype(jnp.float32).astype(jnp.bfloat16)
        one = jnp.ones((), jnp.bfloat16)

        def step(c, carry):
            left, right = [], []
            for j in range(depth):
                at = pl.ds(pl.multiple_of((c * depth + j) * 16, 16), 16)
                lo = lo_b[at, :]
                high = hi_b[at, :] * jnp.bfloat16(both // side) + part_b[at, :] * jnp.bfloat16(width // side)
                step = width // 2
                while step >= side:
                    over = lo >= jnp.bfloat16(step)
                    lo = jnp.where(over, lo - jnp.bfloat16(step), lo)
                    high = jnp.where(over, high + jnp.bfloat16(step // side), high)
                    step //= 2
                w = w_b[at, :]
                left.append(jnp.where(jnp.concatenate([high] * (per_row // 16), axis=0) == high_label,
                                      jnp.concatenate([w] * (per_row // 16), axis=0), zero))
                right.append(jnp.where(jnp.concatenate([lo] * (side // 16), axis=0) == low_label, one, zero))
            return carry + lax.dot_general(jnp.concatenate(left, axis=1), jnp.concatenate(right, axis=1),
                                           (((1,), (1,)), ((), ())), preferred_element_type=jnp.float32)

        found = lax.fori_loop(0, rows // depth, step, jnp.zeros((per_row, side), jnp.float32))
        found = jnp.concatenate([found[0:per_row // 2], found[per_row // 2:]], axis=1)
        for t in range(BINS // LANES):
            mass_tab[t] = jnp.broadcast_to(found[t:t + 1], (8, LANES))

    def remote(src, dst, ss, rs, chip_to, core_to):
        return pltpu.make_async_remote_copy(src, dst, ss, rs, device_id={"dom": chip_to * 2 + core_to},
                                            device_id_type=pl.DeviceIdType.MESH)

    def rows_of(table, dest, which):
        found = [table[(dest * 2 + which) * chunks + j][0:1] for j in range(chunks)]
        pad = [jnp.zeros((4 - chunks, LANES), jnp.float32)] if chunks < 4 else []
        return jnp.concatenate(found + pad, axis=0)

    def table_copy(which):
        src, dst = ((tops_send, tops_recv), (mass_send, mass_recv))[which]
        return remote(src, dst, table_ss.at[which], table_rs.at[which], chip, 1 - core)

    def pair_copy(u):
        return remote(pair_send.at[u], pair_recv.at[u], pair_ss.at[u], pair_rs.at[u], chip, 1 - core)

    def piece(p):
        return pl.ds(pl.multiple_of(p * per * state, per * state), per * state)

    def chunk(j):
        return pl.ds(pl.multiple_of(j * state, state), state)

    def incoming(slot, p):
        return remote(send.at[0, piece(p)], recv.at[slot, piece(p)], chip_ss.at[0], chip_rs.at[slot, p], chip, 1 - core)

    def incoming_word(slot):
        return remote(send_s.at[0], recv_s.at[slot], word_ss.at[0], word_rs.at[slot], chip, 1 - core)

    def at_step(values, s):
        found = values[0]
        for k in range(1, len(values)):
            found = found + jnp.where(s == k, values[k] - values[0], 0)
        return found

    targets = [pick([t[s] for t in target], chip) for s in range(last)]
    slots = [chip + pick([m[s] for m in merged], chip) * (chips - chip) for s in range(last)]

    def outgoing(u):
        s, p = u // half, u % half
        return remote(send.at[s, piece(p)], recv.at[at_step(slots, s), piece(p)], chip_ss.at[u],
                      chip_rs.at[at_step(slots, s), p], at_step(targets, s), core)

    def outgoing_word(s):
        return remote(send_s.at[s], recv_s.at[slots[s]], word_ss.at[s], word_rs.at[slots[s]], targets[s], core)

    def merges(s):
        first, final = merging[s]
        return (chip >= first) & (chip <= final)

    def give(u):
        found = blocks[u % 2, pl.ds(pl.multiple_of((1 - core) * state, state), state)]
        for l in range(per):
            pair_send[u, l * state:(l + 1) * state] = found[:, l * LANES:(l + 1) * LANES]
        pair_copy(u).start()

    def keep(table, s, values):
        for j in range(chunks):
            table[s * chunks + j] = jnp.broadcast_to(values[j:j + 1], (8, LANES))

    def handle_tops():
        table_copy(0).wait_recv()
        for s in range(chips):
            mine, theirs = rows_of(top_tab, dests[s], core), tops_recv[s]
            most = jnp.maximum(mine, theirs)
            keep(by_mine, s, jnp.exp(mine - most))
            keep(by_theirs, s, jnp.exp(theirs - most))
            send_s[s, 4:8] = most

    def handle_masses():
        table_copy(1).wait_recv()
        for s in range(chips):
            for j in range(chunks):
                mine = mass_tab[(dests[s] * 2 + core) * chunks + j][0:1]
                send_s[s, j:j + 1] = (mine * by_mine[s * chunks + j, 0:1]
                                      + mass_recv[s, j:j + 1] * by_theirs[s * chunks + j, 0:1])
            for j in range(chunks, 4):
                send_s[s, j:j + 1] = jnp.zeros((1, LANES), jnp.float32)
            if s < last and s not in merging:
                outgoing_word(s).start()

    def scale_step(s, values):
        for j in range(chunks):
            by_mine[s * chunks + j] = by_mine[s * chunks + j] * values[j:j + 1]
            by_theirs[s * chunks + j] = by_theirs[s * chunks + j] * values[j:j + 1]

    def merge_words(s):
        @pl.when(merges(s))
        def _():
            incoming_word(chips).wait_recv()
            mine, theirs = send_s[s, 4:8], recv_s[chips, 4:8]
            most = jnp.maximum(mine, theirs)
            to_mine, to_theirs = jnp.exp(mine - most), jnp.exp(theirs - most)
            scale_step(s, to_mine)
            keep(fac, chips, to_theirs)
            send_s[s, 0:4] = send_s[s, 0:4] * to_mine + recv_s[chips, 0:4] * to_theirs
            send_s[s, 4:8] = most

        outgoing_word(s).start()

    def handle(u):
        s, p = u // half, u % half
        for m in merging:
            @pl.when(u == m * half)
            def _(m=m):
                merge_words(m)
        pair_copy(u).wait_recv()
        found = blocks[u % 2, pl.ds(pl.multiple_of(core * state, state), state)]
        for l in range(per):
            j = p * per + l
            send[s, chunk(j)] = (
                found[:, l * LANES:(l + 1) * LANES] * by_mine[s * chunks + j, 0:1]
                + pair_recv[u, l * state:(l + 1) * state] * by_theirs[s * chunks + j, 0:1])
        for m in merging:
            @pl.when((s == m) & merges(m))
            def _(m=m):
                incoming(chips, p).wait_recv()
                for l in range(per):
                    j = p * per + l
                    send[m, chunk(j)] = send[m, chunk(j)] + recv[chips, chunk(j)] * fac[chips * chunks + j, 0:1]

        @pl.when(s < last)
        def _():
            outgoing(u).start()

    def valid(sender):
        ok = chip != sender
        for owner, other in skipped:
            if other == sender:
                ok = ok & (chip != owner)
        return ok

    real = lax.broadcasted_iota(jnp.int32, (4, LANES), 0) < chunks

    def stat_copies():
        return [pltpu.make_async_remote_copy(
            stat_send, stat_recv.at[k - 1], stat_ss.at[k - 1], stat_rs.at[k - 1],
            device_id={"dom": lax.rem(me + k, groups)}, device_id_type=pl.DeviceIdType.MESH)
            for k in range(1, groups)]

    def owned_words():
        for c in range(chips):
            @pl.when(valid(c))
            def _(c=c):
                incoming_word(c).wait_recv()

            @pl.when(jnp.logical_not(valid(c)))
            def _(c=c):
                recv_s[c, 0:4] = jnp.zeros((4, LANES), jnp.float32)
                recv_s[c, 4:8] = jnp.full((4, LANES), floor_value, jnp.float32)

        own = send_s[last, 4:8]
        bin_top = own
        for c in range(chips):
            bin_top = jnp.maximum(bin_top, recv_s[c, 4:8])
        by_own = jnp.exp(own - bin_top)
        mass = send_s[last, 0:4] * by_own
        for c in range(chips):
            by = jnp.exp(recv_s[c, 4:8] - bin_top)
            keep(fac, c, by)
            mass = mass + recv_s[c, 0:4] * by
        scale_step(last, by_own)
        block_top = jnp.max(jnp.max(jnp.where(real, bin_top, floor_value), axis=1, keepdims=True), axis=0,
                            keepdims=True)
        share = jnp.where(real, mass * jnp.exp(bin_top - block_top), 0.0)
        block_mass = jnp.sum(jnp.sum(share, axis=1, keepdims=True), axis=0, keepdims=True)
        send_s[last, 0:4] = mass
        send_s[last, 4:8] = share
        stat_send[0:4, :] = jnp.broadcast_to(block_top, (4, LANES))
        stat_send[4:8, :] = jnp.broadcast_to(block_mass, (4, LANES))
        for copy in stat_copies():
            copy.start()

    def close_stats():
        share = send_s[last, 4:8]
        run = share
        position = lax.broadcasted_iota(jnp.int32, run.shape, 1)
        hop = 1
        while hop < LANES:
            run = run + jnp.where(position >= hop, pltpu.roll(run, hop, 1), 0.0)
            hop *= 2
        base = jnp.zeros((1, 1), jnp.float32)
        runs = []
        for j in range(chunks):
            runs.append(run[j:j + 1] + base)
            base = base + run[j:j + 1, LANES - 1:LANES]
        for copy in stat_copies():
            copy.wait_recv()
        block_top, block_mass = stat_send[0:1, 0:1], stat_send[4:5, 0:1]
        top = block_top
        for k in range(groups - 1):
            top = jnp.maximum(top, stat_recv[k, 0:1, 0:1])
        scale = jnp.exp(block_top - top)
        total = block_mass * scale
        before = jnp.zeros_like(total)
        for k in range(groups - 1):
            theirs = stat_recv[k, 4:5, 0:1] * jnp.exp(stat_recv[k, 0:1, 0:1] - top)
            total = total + theirs
            before = before + jnp.where(me >= k + 1, theirs, 0.0)
        cum_ref[...] = (before + jnp.concatenate(runs, axis=1) * scale) / total
        weights_ref[...] = whole_count * jnp.exp(lw_ref[...] - top) / total

    for s in range(chips):
        tops_send[s] = rows_of(top_tab, dests[s], 1 - core)
    mask_states(0)
    pl.semaphore_wait(barrier, groups - 1)
    table_copy(0).start()
    depth = min(64, rows) if chips <= 4 else min(16, rows)
    steps = rows // depth

    def turn(v, carry):
        u, c = v // steps, v % steps
        s, p = u // half, u % half
        found = blocks.at[u % 2]
        added = product(at_step(dests, s), p, c, depth)

        found[...] = jnp.where(c > 0, found[...], 0.0) + added

        @pl.when(v == 2 * steps - 1)
        def _():
            handle_masses()

        @pl.when(v == (units - 1) * steps)
        def _():
            owned_words()

        @pl.when((c == 0) & (u > 1))
        def _():
            handle(u - 1)

        @pl.when(c == steps - 1)
        def _():
            give(u)

        @pl.when(v == steps - 1)
        def _():
            for q in range(1, half):
                mask_states(q)
            mass_table()
            for t in range(chips):
                mass_send[t] = rows_of(mass_tab, dests[t], 1 - core)
            table_copy(1).start()
            handle_tops()
            handle(0)

        return carry

    lax.fori_loop(0, units * steps, turn, 0)
    handle(units - 1)
    close_stats()
    for c in range(chips):
        @pl.when(valid(c))
        def _(c=c):
            for p in range(half):
                incoming(c, p).wait_recv()
            for j in range(chunks):
                at = slice(j * state, (j + 1) * state)
                send[last, at] = send[last, at] + recv[c, at] * fac[c * chunks + j, 0:1]
    for j in range(chunks):
        means_ref[:, j * LANES:(j + 1) * LANES] = (send[last, j * state:(j + 1) * state]
                                                   / jnp.maximum(send_s[last, j:j + 1], 1.0))
    for which in range(2):
        table_copy(which).wait_send()
    for u in range(units):
        pair_copy(u).wait_send()
    for u in range(last * half):
        outgoing(u).wait_send()
    for s in range(last):
        outgoing_word(s).wait_send()
    for copy in stat_copies():
        copy.wait_send()


def drain(*refs):
    sources, results, sems = refs[0:3], refs[3:6], refs[6]
    copies = [pltpu.make_async_copy(sources[i], results[i], sems.at[i]) for i in range(3)]
    for copy in copies:
        copy.start()
    for copy in copies:
        copy.wait()


def body(log_weights, bins, states):
    groups = lax.axis_size("dom")
    owned = BINS // groups
    chips = groups // 2
    state, count = states.shape
    rows = count // LANES
    width = min(256, owned)
    chunks = owned // LANES
    vmem = pl.BlockSpec(memory_space=pltpu.VMEM)
    hbm = pl.BlockSpec(memory_space=pltpu.HBM)

    half = owned // width
    units = chips * half

    def sums(slots):
        return pltpu.VMEM((slots, chunks * state, LANES), jnp.float32)

    def words(slots, depth=8):
        return pltpu.VMEM((slots, depth, LANES), jnp.float32)

    def spread():
        return pltpu.VMEM((rows * 16, LANES), jnp.bfloat16)

    shapes = (jax.ShapeDtypeStruct((1, owned), jnp.float32),
              jax.ShapeDtypeStruct((state, owned), jnp.float32),
              jax.ShapeDtypeStruct((rows, LANES), jnp.float32))
    found = pl.pallas_call(
        functools.partial(kernel, groups, float(count * groups)),
        out_shape=shapes,
        in_specs=[vmem, vmem, hbm],
        out_specs=(vmem, vmem, vmem),
        scratch_shapes=[
            pltpu.VMEM((state, count), jnp.bfloat16),
            pltpu.VMEM((rows, 2 * half * state, LANES), jnp.bfloat16),
            spread(), spread(), spread(), spread(),
            words(BINS // LANES), words(BINS // LANES),
            pltpu.VMEM((2, 2 * state, width), jnp.float32),
            words(chips, 4), words(chips, 4), words(chips, 4), words(chips, 4),
            pltpu.VMEM((units, (width // LANES) * state, LANES), jnp.float32),
            pltpu.VMEM((units, (width // LANES) * state, LANES), jnp.float32),
            words(chips * chunks), words(chips * chunks),
            sums(chips), sums(chips + 1), words(chips), words(chips + 1), words((chips + 1) * chunks),
            pltpu.VMEM((8, LANES), jnp.float32),
            words(groups - 1),
            pltpu.SemaphoreType.DMA,
            pltpu.SemaphoreType.DMA((2,)),
            pltpu.SemaphoreType.DMA((2,)),
            pltpu.SemaphoreType.DMA((units,)),
            pltpu.SemaphoreType.DMA((units,)),
            pltpu.SemaphoreType.DMA((units,)),
            pltpu.SemaphoreType.DMA((chips + 1, half)),
            pltpu.SemaphoreType.DMA((chips,)),
            pltpu.SemaphoreType.DMA((chips + 1,)),
            pltpu.SemaphoreType.DMA((groups - 1,)),
            pltpu.SemaphoreType.DMA((groups - 1,)),
        ],
        compiler_params=pltpu.CompilerParams(
            collective_id=0, has_side_effects=True, vmem_limit_bytes=52 * 1024 * 1024),
    )(log_weights.reshape(rows, LANES), bins.reshape(rows, LANES), states)
    cumulative, bin_means, weights = pl.pallas_call(
        drain,
        out_shape=shapes,
        in_specs=[vmem, vmem, vmem],
        out_specs=(hbm, hbm, hbm),
        scratch_shapes=[pltpu.SemaphoreType.DMA((3,))],
        compiler_params=pltpu.CompilerParams(vmem_limit_bytes=4 * 1024 * 1024),
    )(*found)
    return cumulative.reshape(owned), bin_means, weights.reshape(count)


def solution(mesh):
    placed = (P(("filt", "dom")), P(("filt", "dom")), P(None, ("filt", "dom")))
    return jax.shard_map(
        body,
        mesh=mesh,
        in_specs=placed,
        out_specs=(P(("filt", "dom")), P(None, ("filt", "dom")), P(("filt", "dom"))),
        check_vma=False,
    )
```

```python
import functools

import jax
import jax.numpy as jnp
from jax import lax
from jax.experimental import pallas as pl
from jax.experimental.pallas import tpu as pltpu
from jax.sharding import PartitionSpec as P

BINS = 4096
LANES = 128
LEVEL_BITS = 20
LEVELS = 1 << LEVEL_BITS
LEAST = -20.0
PER_UNIT = (LEVELS - 3) / 270.0

floor_value = -10000.0


def spread_rows(ref, values):
    for r in range(values.shape[0]):
        ref[16 * r:16 * r + 16, :] = jnp.broadcast_to(values[r:r + 1, :], (16, LANES)).astype(ref.dtype)


def sort_keys(keys):
    tile_bits = len(keys).bit_length() - 1
    bits = tile_bits + 10
    sub = lax.broadcasted_iota(jnp.int32, (8, LANES), 0)
    lane = lax.broadcasted_iota(jnp.int32, (8, LANES), 1)

    def mask_of(bit):
        if bit < tile_bits + 3:
            return (sub >> (bit - tile_bits)) & 1
        return (lane >> (bit - tile_bits - 3)) & 1

    def turned(size):
        if size >= bits:
            return None
        if size < tile_bits:
            return [-((t >> size) & 1) for t in range(len(keys))]
        return -mask_of(size)

    def flip(now, then):
        for t in range(len(keys)):
            a = now[t] if isinstance(now, list) else now
            b = then[t] if isinstance(then, list) else then
            if a is None:
                a = 0
            if b is None:
                b = 0
            if isinstance(a, int) and isinstance(b, int):
                if a != b:
                    keys[t] = ~keys[t]
                continue
            keys[t] = keys[t] ^ (a ^ b)

    before = None
    for size in range(1, bits + 1):
        down = turned(size)
        flip(before, down)
        before = down
        for bit in range(size - 1, -1, -1):
            if bit < tile_bits:
                for t in range(len(keys)):
                    o = t | (1 << bit)
                    if o != t:
                        keys[t], keys[o] = jnp.minimum(keys[t], keys[o]), jnp.maximum(keys[t], keys[o])
                continue
            upper = mask_of(bit) != 0
            if bit < tile_bits + 3:
                index, axis = sub ^ (1 << (bit - tile_bits)), 0
            else:
                index, axis = lane ^ (1 << (bit - tile_bits - 3)), 1
            for t in range(len(keys)):
                k = jnp.take_along_axis(keys[t], index, axis=axis)
                keys[t] = jnp.where(upper, jnp.maximum(keys[t], k), jnp.minimum(keys[t], k))
    return keys


def local_tops(lw, bins):
    count = lw.shape[0] // 8
    table = BINS // LANES
    level = jnp.clip((lw - LEAST) * PER_UNIT + 1.5, 1.0, float(LEVELS - 1)).astype(jnp.int32)
    packed = (bins - BINS // 2) * LEVELS + level
    keys = sort_keys([packed[8 * t:8 * t + 8] for t in range(count)])
    sub = lax.broadcasted_iota(jnp.int32, (8, LANES), 0)
    lane = lax.broadcasted_iota(jnp.int32, (8, LANES), 1)
    places = [(k >> LEVEL_BITS) + BINS // 2 for k in keys]
    turned = pltpu.roll(places[0], 7, 0)
    following = jnp.where(sub == 7, pltpu.roll(turned, LANES - 1, 1), turned)
    following = jnp.where((sub == 7) & (lane == LANES - 1), -1, following)
    high_label = lax.broadcasted_iota(jnp.int32, (table, LANES), 0).astype(jnp.float32).astype(jnp.bfloat16)
    low_label = lax.broadcasted_iota(jnp.int32, (LANES, LANES), 0).astype(jnp.float32).astype(jnp.bfloat16)
    zero, one = jnp.zeros((), jnp.bfloat16), jnp.ones((), jnp.bfloat16)
    found = jnp.zeros((3 * table, LANES), jnp.float32)

    def row(x, r):
        return jnp.broadcast_to(x[r:r + 1], (16, LANES)).astype(jnp.bfloat16)

    for t in range(count):
        last = places[t] != (places[t + 1] if t + 1 < count else following)
        high = jnp.where(last, places[t] // LANES, -1).astype(jnp.float32)
        low = (places[t] % LANES).astype(jnp.float32)
        size = keys[t] & (LEVELS - 1)
        parts = [(size >> 12).astype(jnp.float32), ((size >> 4) & 255).astype(jnp.float32),
                 (size & 15).astype(jnp.float32)]
        left, right = [], []
        for r in range(8):
            member = jnp.concatenate([row(high, r)] * (table // 16), axis=0) == high_label
            left.append(jnp.concatenate(
                [jnp.where(member, jnp.concatenate([row(x, r)] * (table // 16), axis=0), zero) for x in parts], axis=0))
            right.append(jnp.where(jnp.concatenate([row(low, r)] * (LANES // 16), axis=0) == low_label, one, zero))
        found = found + lax.dot_general(jnp.concatenate(left, axis=1), jnp.concatenate(right, axis=1),
                                        (((1,), (1,)), ((), ())), preferred_element_type=jnp.float32)
    top = (found[0:table] * 4096.0 + found[table:2 * table] * 16.0) + found[2 * table:3 * table]
    return jnp.where(top > 0.5, (top - 1.0) * (1.0 / PER_UNIT) + LEAST, floor_value)


def plan(chips):
    if chips == 4:
        order = [[3, 1, 2, 0], [2, 3, 0, 1], [1, 0, 3, 2], [0, 2, 1, 3]]
        target = [[1, 1, 2], [2, 3, 0], [1, 0, 3], [2, 2, 1]]
        merged = [[1, 0, 0], [0, 0, 0], [0, 0, 0], [1, 0, 0]]
        return order, target, merged, {1: (1, 2)}, {(0, 3), (3, 0)}
    order = [sorted((d for d in range(chips) if d != c), key=lambda d: -abs(d - c)) + [c] for c in range(chips)]
    target = [o[:-1] for o in order]
    merged = [[0] * (chips - 1) for _ in range(chips)]
    return order, target, merged, {}, set()


def pick(table, chip):
    value = table[0]
    for c in range(1, len(table)):
        if table[c] != table[c - 1]:
            value = value + jnp.where(chip >= c, table[c] - table[c - 1], 0)
    return value


def kernel(groups, whole_count, lw_hbm, bins_hbm, states_hbm, cum_ref, means_ref, weights_ref,
           lw_ref, bins_ref, held, ext, lo_b, hi_b, part_b, w_b, top_tab, mass_tab, blocks,
           tops_send, tops_recv, mass_send, mass_recv, pair_recv, by_mine, by_theirs,
           send, recv, send_s, recv_s, fac, stat_send, stat_recv,
           load_sem, table_ss, table_rs, pair_ss, pair_rs, chip_ss, chip_rs, word_ss, word_rs, stat_ss, stat_rs):
    state = held.shape[0]
    count = held.shape[1]
    rows = count // LANES
    owned = BINS // groups
    both = 2 * owned
    width = min(256, owned)
    half = owned // width
    chunks = owned // LANES
    per = width // LANES
    chips = groups // 2
    units = chips * half
    last = chips - 1
    order, target, merged, merging, skipped = plan(chips)
    me = lax.axis_index("dom")
    chip, core = me // 2, me % 2
    dests = [pick([o[s] for o in order], chip) for s in range(chips)]

    loads = [pltpu.make_async_copy(src, dst, load_sem.at[i]) for i, (src, dst) in enumerate(
        ((bins_hbm, bins_ref), (lw_hbm, lw_ref), (states_hbm, held)))]
    for load in loads:
        load.start()
    barrier = pltpu.get_barrier_semaphore()
    for k in range(1, groups):
        pl.semaphore_signal(barrier, inc=1, device_id={"dom": lax.rem(me + k, groups)},
                            device_id_type=pl.DeviceIdType.MESH)

    loads[0].wait()
    loads[1].wait()
    lw = lw_ref[...]
    bins = bins_ref[...]
    spread_rows(lo_b, (bins % width).astype(jnp.float32))
    spread_rows(hi_b, (bins // both).astype(jnp.float32))
    spread_rows(part_b, ((bins % both) // width).astype(jnp.float32))
    tops = local_tops(lw, bins)
    low, high = bins % LANES, bins // LANES
    loads[2].wait()
    zero = jnp.zeros((), jnp.bfloat16)

    def mask_tile(r, p):
        part = part_b[pl.ds(pl.multiple_of(r * 16, 16), 16), :]
        tile = held[:, pl.ds(pl.multiple_of(r * LANES, LANES), LANES)]
        part_all = jnp.concatenate([part] * (state // 16), axis=0)
        for k in range(2):
            at = (2 * p + k) * state
            ext[r, at:at + state] = jnp.where(part_all == jnp.bfloat16(k * half + p), tile, zero)

    own_tops = []
    for v in range(rows // 8):
        at = slice(8 * v, 8 * v + 8)
        found = jnp.zeros((8, LANES), jnp.float32)
        for t in range(BINS // LANES):
            picked = jnp.take_along_axis(jnp.broadcast_to(tops[t:t + 1], (8, LANES)), low[at], axis=1)
            found = jnp.where(high[at] == t, picked, found)
        own_tops.append(found)
        for r in range(8 * v, 8 * v + 8):
            mask_tile(r, 0)
    own_top = jnp.concatenate(own_tops, axis=0)
    for t in range(BINS // LANES):
        top_tab[t] = jnp.broadcast_to(tops[t:t + 1], (8, LANES))
    spread_rows(w_b, jnp.exp(lw - own_top))

    def mask_states(p):
        def step(r, carry):
            for i in range(4):
                mask_tile(4 * r + i, p)
            return carry

        lax.fori_loop(0, rows // 4, step, 0)

    label = lax.broadcasted_iota(jnp.int32, (width, LANES), 0).astype(jnp.float32).astype(jnp.bfloat16)

    def product(dest, p, c, depth):
        tile = jnp.asarray(dest).astype(jnp.float32).astype(jnp.bfloat16)
        pieces = []
        for j in range(depth):
            at = pl.ds(pl.multiple_of((c * depth + j) * 16, 16), 16)
            w = jnp.where(hi_b[at, :] == tile, w_b[at, :], zero)
            lo = lo_b[at, :]
            w_all = jnp.concatenate([w] * (width // 16), axis=0)
            lo_all = jnp.concatenate([lo] * (width // 16), axis=0)
            pieces.append(jnp.where(lo_all == label, w_all, zero))
        spread = jnp.concatenate(pieces, axis=1)
        at = pl.ds(pl.multiple_of(2 * p * state, 2 * state), 2 * state)
        left = jnp.concatenate([ext[c * depth + j, at] for j in range(depth)], axis=1)
        return lax.dot_general(left, spread, (((1,), (1,)), ((), ())), preferred_element_type=jnp.float32)

    def mass_table():
        side = 64
        depth = min(64, rows)
        per_row = BINS // side
        low_label = lax.broadcasted_iota(jnp.int32, (side, LANES), 0).astype(jnp.float32).astype(jnp.bfloat16)
        turn = lax.broadcasted_iota(jnp.int32, (per_row, LANES), 0)
        turn = 2 * (turn % (per_row // 2)) + turn // (per_row // 2)
        high_label = turn.astype(jnp.float32).astype(jnp.bfloat16)
        one = jnp.ones((), jnp.bfloat16)

        def step(c, carry):
            left, right = [], []
            for j in range(depth):
                at = pl.ds(pl.multiple_of((c * depth + j) * 16, 16), 16)
                lo = lo_b[at, :]
                high = hi_b[at, :] * jnp.bfloat16(both // side) + part_b[at, :] * jnp.bfloat16(width // side)
                step = width // 2
                while step >= side:
                    over = lo >= jnp.bfloat16(step)
                    lo = jnp.where(over, lo - jnp.bfloat16(step), lo)
                    high = jnp.where(over, high + jnp.bfloat16(step // side), high)
                    step //= 2
                w = w_b[at, :]
                left.append(jnp.where(jnp.concatenate([high] * (per_row // 16), axis=0) == high_label,
                                      jnp.concatenate([w] * (per_row // 16), axis=0), zero))
                right.append(jnp.where(jnp.concatenate([lo] * (side // 16), axis=0) == low_label, one, zero))
            return carry + lax.dot_general(jnp.concatenate(left, axis=1), jnp.concatenate(right, axis=1),
                                           (((1,), (1,)), ((), ())), preferred_element_type=jnp.float32)

        found = lax.fori_loop(0, rows // depth, step, jnp.zeros((per_row, side), jnp.float32))
        found = jnp.concatenate([found[0:per_row // 2], found[per_row // 2:]], axis=1)
        for t in range(BINS // LANES):
            mass_tab[t] = jnp.broadcast_to(found[t:t + 1], (8, LANES))

    def remote(src, dst, ss, rs, chip_to, core_to):
        return pltpu.make_async_remote_copy(src, dst, ss, rs, device_id={"dom": chip_to * 2 + core_to},
                                            device_id_type=pl.DeviceIdType.MESH)

    def rows_of(table, dest, which):
        found = [table[(dest * 2 + which) * chunks + j][0:1] for j in range(chunks)]
        pad = [jnp.zeros((4 - chunks, LANES), jnp.float32)] if chunks < 4 else []
        return jnp.concatenate(found + pad, axis=0)

    def table_copy(which):
        src, dst = ((tops_send, tops_recv), (mass_send, mass_recv))[which]
        return remote(src, dst, table_ss.at[which], table_rs.at[which], chip, 1 - core)

    def pair_copy(u):
        theirs = blocks.at[u, pl.ds(pl.multiple_of((1 - core) * state, state), state)]
        return remote(theirs, pair_recv.at[u], pair_ss.at[u], pair_rs.at[u], chip, 1 - core)

    def piece(p):
        return pl.ds(pl.multiple_of(p * per * state, per * state), per * state)

    def chunk(j):
        return pl.ds(pl.multiple_of(j * state, state), state)

    def incoming(slot, p):
        return remote(send.at[0, piece(p)], recv.at[slot, piece(p)], chip_ss.at[0], chip_rs.at[slot, p], chip, 1 - core)

    def incoming_word(slot):
        return remote(send_s.at[0], recv_s.at[slot], word_ss.at[0], word_rs.at[slot], chip, 1 - core)

    def at_step(values, s):
        found = values[0]
        for k in range(1, len(values)):
            found = found + jnp.where(s == k, values[k] - values[0], 0)
        return found

    targets = [pick([t[s] for t in target], chip) for s in range(last)]
    slots = [chip + pick([m[s] for m in merged], chip) * (chips - chip) for s in range(last)]

    def outgoing(u):
        s, p = u // half, u % half
        return remote(send.at[s, piece(p)], recv.at[at_step(slots, s), piece(p)], chip_ss.at[u],
                      chip_rs.at[at_step(slots, s), p], at_step(targets, s), core)

    def outgoing_word(s):
        return remote(send_s.at[s], recv_s.at[slots[s]], word_ss.at[s], word_rs.at[slots[s]], targets[s], core)

    def merges(s):
        first, final = merging[s]
        return (chip >= first) & (chip <= final)

    def give(u):
        pair_copy(u).start()

    def keep(table, s, values):
        for j in range(chunks):
            table[s * chunks + j] = jnp.broadcast_to(values[j:j + 1], (8, LANES))

    def handle_tops():
        table_copy(0).wait_recv()
        for s in range(chips):
            mine, theirs = rows_of(top_tab, dests[s], core), tops_recv[s]
            most = jnp.maximum(mine, theirs)
            keep(by_mine, s, jnp.exp(mine - most))
            keep(by_theirs, s, jnp.exp(theirs - most))
            send_s[s, 4:8] = most

    def handle_masses():
        table_copy(1).wait_recv()
        for s in range(chips):
            for j in range(chunks):
                mine = mass_tab[(dests[s] * 2 + core) * chunks + j][0:1]
                send_s[s, j:j + 1] = (mine * by_mine[s * chunks + j, 0:1]
                                      + mass_recv[s, j:j + 1] * by_theirs[s * chunks + j, 0:1])
            for j in range(chunks, 4):
                send_s[s, j:j + 1] = jnp.zeros((1, LANES), jnp.float32)
            if s < last and s not in merging:
                outgoing_word(s).start()

    def scale_step(s, values):
        for j in range(chunks):
            by_mine[s * chunks + j] = by_mine[s * chunks + j] * values[j:j + 1]
            by_theirs[s * chunks + j] = by_theirs[s * chunks + j] * values[j:j + 1]

    def merge_words(s):
        @pl.when(merges(s))
        def _():
            incoming_word(chips).wait_recv()
            mine, theirs = send_s[s, 4:8], recv_s[chips, 4:8]
            most = jnp.maximum(mine, theirs)
            to_mine, to_theirs = jnp.exp(mine - most), jnp.exp(theirs - most)
            scale_step(s, to_mine)
            keep(fac, chips, to_theirs)
            send_s[s, 0:4] = send_s[s, 0:4] * to_mine + recv_s[chips, 0:4] * to_theirs
            send_s[s, 4:8] = most

        outgoing_word(s).start()

    def handle(u):
        s, p = u // half, u % half
        for m in merging:
            @pl.when(u == m * half)
            def _(m=m):
                merge_words(m)
        pair_copy(u).wait_recv()
        found = blocks[u, pl.ds(pl.multiple_of(core * state, state), state)]
        for l in range(per):
            j = p * per + l
            send[s, chunk(j)] = (
                found[:, l * LANES:(l + 1) * LANES] * by_mine[s * chunks + j, 0:1]
                + pair_recv[u, :, l * LANES:(l + 1) * LANES] * by_theirs[s * chunks + j, 0:1])
        for m in merging:
            @pl.when((s == m) & merges(m))
            def _(m=m):
                incoming(chips, p).wait_recv()
                for l in range(per):
                    j = p * per + l
                    send[m, chunk(j)] = send[m, chunk(j)] + recv[chips, chunk(j)] * fac[chips * chunks + j, 0:1]

        @pl.when(s < last)
        def _():
            outgoing(u).start()

    def valid(sender):
        ok = chip != sender
        for owner, other in skipped:
            if other == sender:
                ok = ok & (chip != owner)
        return ok

    real = lax.broadcasted_iota(jnp.int32, (4, LANES), 0) < chunks

    def stat_copies():
        return [pltpu.make_async_remote_copy(
            stat_send, stat_recv.at[k - 1], stat_ss.at[k - 1], stat_rs.at[k - 1],
            device_id={"dom": lax.rem(me + k, groups)}, device_id_type=pl.DeviceIdType.MESH)
            for k in range(1, groups)]

    def owned_words():
        for c in range(chips):
            @pl.when(valid(c))
            def _(c=c):
                incoming_word(c).wait_recv()

            @pl.when(jnp.logical_not(valid(c)))
            def _(c=c):
                recv_s[c, 0:4] = jnp.zeros((4, LANES), jnp.float32)
                recv_s[c, 4:8] = jnp.full((4, LANES), floor_value, jnp.float32)

        own = send_s[last, 4:8]
        bin_top = own
        for c in range(chips):
            bin_top = jnp.maximum(bin_top, recv_s[c, 4:8])
        by_own = jnp.exp(own - bin_top)
        mass = send_s[last, 0:4] * by_own
        for c in range(chips):
            by = jnp.exp(recv_s[c, 4:8] - bin_top)
            keep(fac, c, by)
            mass = mass + recv_s[c, 0:4] * by
        scale_step(last, by_own)
        block_top = jnp.max(jnp.max(jnp.where(real, bin_top, floor_value), axis=1, keepdims=True), axis=0,
                            keepdims=True)
        share = jnp.where(real, mass * jnp.exp(bin_top - block_top), 0.0)
        block_mass = jnp.sum(jnp.sum(share, axis=1, keepdims=True), axis=0, keepdims=True)
        send_s[last, 0:4] = mass
        send_s[last, 4:8] = share
        stat_send[0:4, :] = jnp.broadcast_to(block_top, (4, LANES))
        stat_send[4:8, :] = jnp.broadcast_to(block_mass, (4, LANES))
        for copy in stat_copies():
            copy.start()

    def close_stats():
        share = send_s[last, 4:8]
        run = share
        position = lax.broadcasted_iota(jnp.int32, run.shape, 1)
        hop = 1
        while hop < LANES:
            run = run + jnp.where(position >= hop, pltpu.roll(run, hop, 1), 0.0)
            hop *= 2
        base = jnp.zeros((1, 1), jnp.float32)
        runs = []
        for j in range(chunks):
            runs.append(run[j:j + 1] + base)
            base = base + run[j:j + 1, LANES - 1:LANES]
        for copy in stat_copies():
            copy.wait_recv()
        block_top, block_mass = stat_send[0:1, 0:1], stat_send[4:5, 0:1]
        top = block_top
        for k in range(groups - 1):
            top = jnp.maximum(top, stat_recv[k, 0:1, 0:1])
        scale = jnp.exp(block_top - top)
        total = block_mass * scale
        before = jnp.zeros_like(total)
        for k in range(groups - 1):
            theirs = stat_recv[k, 4:5, 0:1] * jnp.exp(stat_recv[k, 0:1, 0:1] - top)
            total = total + theirs
            before = before + jnp.where(me >= k + 1, theirs, 0.0)
        cum_ref[...] = (before + jnp.concatenate(runs, axis=1) * scale) / total
        weights_ref[...] = whole_count * jnp.exp(lw_ref[...] - top) / total

    for s in range(chips):
        tops_send[s] = rows_of(top_tab, dests[s], 1 - core)
    pl.semaphore_wait(barrier, groups - 1)
    table_copy(0).start()
    depth = min(64, rows) if chips <= 4 else min(16, rows)
    steps = rows // depth

    def turn(v, carry):
        u, c = v // steps, v % steps
        s, p = u // half, u % half
        found = blocks.at[u]
        added = product(at_step(dests, s), p, c, depth)

        found[...] = jnp.where(c > 0, found[...], 0.0) + added

        @pl.when(v == 2 * steps - 1)
        def _():
            handle_masses()

        @pl.when(v == (units - 1) * steps)
        def _():
            owned_words()

        @pl.when((c == 0) & (u > 1))
        def _():
            handle(u - 1)

        @pl.when(c == steps - 1)
        def _():
            give(u)

        @pl.when(v == steps - 1)
        def _():
            for q in range(1, half):
                mask_states(q)
            mass_table()
            for t in range(chips):
                mass_send[t] = rows_of(mass_tab, dests[t], 1 - core)
            table_copy(1).start()
            handle_tops()
            handle(0)

        return carry

    lax.fori_loop(0, units * steps, turn, 0)
    close_stats()
    for p in range(half):
        if p == half - 1:
            handle(units - 1)
        for c in range(chips):
            @pl.when(valid(c))
            def _(c=c, p=p):
                incoming(c, p).wait_recv()
                for j in range(p * per, (p + 1) * per):
                    at = slice(j * state, (j + 1) * state)
                    send[last, at] = send[last, at] + recv[c, at] * fac[c * chunks + j, 0:1]
    for j in range(chunks):
        means_ref[:, j * LANES:(j + 1) * LANES] = (send[last, j * state:(j + 1) * state]
                                                   / jnp.maximum(send_s[last, j:j + 1], 1.0))
    for which in range(2):
        table_copy(which).wait_send()
    for u in range(units):
        pair_copy(u).wait_send()
    for u in range(last * half):
        outgoing(u).wait_send()
    for s in range(last):
        outgoing_word(s).wait_send()
    for copy in stat_copies():
        copy.wait_send()


def drain(*refs):
    sources, results, sems = refs[0:3], refs[3:6], refs[6]
    copies = [pltpu.make_async_copy(sources[i], results[i], sems.at[i]) for i in range(3)]
    for copy in copies:
        copy.start()
    for copy in copies:
        copy.wait()


def body(log_weights, bins, states):
    groups = lax.axis_size("dom")
    owned = BINS // groups
    chips = groups // 2
    state, count = states.shape
    rows = count // LANES
    width = min(256, owned)
    chunks = owned // LANES
    vmem = pl.BlockSpec(memory_space=pltpu.VMEM)
    hbm = pl.BlockSpec(memory_space=pltpu.HBM)

    half = owned // width
    units = chips * half

    def sums(slots):
        return pltpu.VMEM((slots, chunks * state, LANES), jnp.float32)

    def words(slots, depth=8):
        return pltpu.VMEM((slots, depth, LANES), jnp.float32)

    def spread():
        return pltpu.VMEM((rows * 16, LANES), jnp.bfloat16)

    shapes = (jax.ShapeDtypeStruct((1, owned), jnp.float32),
              jax.ShapeDtypeStruct((state, owned), jnp.float32),
              jax.ShapeDtypeStruct((rows, LANES), jnp.float32))
    found = pl.pallas_call(
        functools.partial(kernel, groups, float(count * groups)),
        out_shape=shapes,
        in_specs=[hbm, hbm, hbm],
        out_specs=(vmem, vmem, vmem),
        scratch_shapes=[
            pltpu.VMEM((rows, LANES), jnp.float32),
            pltpu.VMEM((rows, LANES), jnp.int32),
            pltpu.VMEM((state, count), jnp.bfloat16),
            pltpu.VMEM((rows, 2 * half * state, LANES), jnp.bfloat16),
            spread(), spread(), spread(), spread(),
            words(BINS // LANES), words(BINS // LANES),
            pltpu.VMEM((units, 2 * state, width), jnp.float32),
            words(chips, 4), words(chips, 4), words(chips, 4), words(chips, 4),
            pltpu.VMEM((units, state, width), jnp.float32),
            words(chips * chunks), words(chips * chunks),
            sums(chips), sums(chips + 1), words(chips), words(chips + 1), words((chips + 1) * chunks),
            pltpu.VMEM((8, LANES), jnp.float32),
            words(groups - 1),
            pltpu.SemaphoreType.DMA((3,)),
            pltpu.SemaphoreType.DMA((2,)),
            pltpu.SemaphoreType.DMA((2,)),
            pltpu.SemaphoreType.DMA((units,)),
            pltpu.SemaphoreType.DMA((units,)),
            pltpu.SemaphoreType.DMA((units,)),
            pltpu.SemaphoreType.DMA((chips + 1, half)),
            pltpu.SemaphoreType.DMA((chips,)),
            pltpu.SemaphoreType.DMA((chips + 1,)),
            pltpu.SemaphoreType.DMA((groups - 1,)),
            pltpu.SemaphoreType.DMA((groups - 1,)),
        ],
        compiler_params=pltpu.CompilerParams(
            collective_id=0, has_side_effects=True, vmem_limit_bytes=52 * 1024 * 1024),
    )(*[pltpu.with_memory_space_constraint(x, pltpu.HBM)
        for x in (log_weights.reshape(rows, LANES), bins.reshape(rows, LANES), states)])
    cumulative, bin_means, weights = pl.pallas_call(
        drain,
        out_shape=shapes,
        in_specs=[vmem, vmem, vmem],
        out_specs=(hbm, hbm, hbm),
        scratch_shapes=[pltpu.SemaphoreType.DMA((3,))],
        compiler_params=pltpu.CompilerParams(vmem_limit_bytes=4 * 1024 * 1024),
    )(*found)
    return cumulative.reshape(owned), bin_means, weights.reshape(count)


def solution(mesh):
    placed = (P(("filt", "dom")), P(("filt", "dom")), P(None, ("filt", "dom")))
    return jax.shard_map(
        body,
        mesh=mesh,
        in_specs=placed,
        out_specs=(P(("filt", "dom")), P(None, ("filt", "dom")), P(("filt", "dom"))),
        check_vma=False,
    )
```
